32 devices in a mesh: groups: 2 (over x), ep: 8 (over z, y), rep: 2 (over core).
Axes of the slice: x: 2, y: 2, z: 4, core: 2. Of those that a mesh axis runs over, the one named last changes fastest.
Arguments:
- tokens: bfloat16 [512, 3584], P(('groups', 'ep'), 'rep'), parts along dimension 0, may hold values from -6 to 6
- expert_ids: int32 [512, 1], P(('groups', 'ep')), parts along dimension 0, may hold values from 0 to 3; in each aligned block of 32 rows (0 to 31, 32 to 63, ...) at most 10 rows name the same one
- gate_values: float32 [512, 1], P(('groups', 'ep')), parts along dimension 0, may hold values from 0.1 to 0.6
- slot_expert: int32 [8], replicated, may hold values from 0 to 3, as said below
- gate_weight: bfloat16 [8, 3584, 1024], P('ep', None, 'rep'), as said below
- up_weight: bfloat16 [8, 3584, 1024], P('ep', None, 'rep'), as said below
- down_weight: bfloat16 [8, 1024, 3584], P('ep', 'rep'), as said below
Outputs:
- combined: bfloat16 [512, 3584], P(('groups', 'ep'), 'rep'), parts along dimension 0
The draws below stay inside these ranges and needn't reach their ends.
There are 2 independent parts, one for each index of `groups`. The reference program is written for one: setup_inputs(seed, part) draws one part's arguments, and reference() takes and returns one part's arrays. A program takes and returns all parts, laid end to end along the dimension named above; an argument that names none is the same for every part. Nothing has to cross between parts.
Inputs may be any that keep to these rules, and one draw needn't show every extreme that they name: `expert_ids`: each row names 1 different experts. Among the 32 rows of one index of ep (aligned blocks) no expert is named more than 10 times, and in some blocks one expert is named exactly 10 times. `slot_expert`: every expert is held by 1 to 4 slots, and some experts by 4. gate_weight[s] equals gate_weight[r] whenever slot_expert[s] equals slot_expert[r]. up_weight[s] equals up_weight[r] whenever slot_expert[s] equals slot_expert[r]. down_weight[s] equals down_weight[r] whenever slot_expert[s] equals slot_expert[r].
All inputs are finite; a program needn't handle non-finite values.
Results may differ from the reference program's by a relative error of at most 0.0057.
Values may be sent and summed in bfloat16 or wider, within the bound.
No kernel may reach another device: no remote copies, remote signals or barrier semaphores. Data moves between devices by JAX's collectives and lax.ppermute only.
A program may use at most 128 MiB of HBM per device.

```python
import math
import jax
import jax.numpy as jnp
import numpy as np
from jax import lax

D = 3584
HID = 1024
TOK_EP = 32
EXPERTS = 4
TOP = 1
CAP = 10
TOKENS = 256
N_EP = 8


def plan_of(key):
    plan_key = jax.random.fold_in(key, 11)
    first_key, second_key = jax.random.split(plan_key)
    ordering = jax.random.permutation(first_key, EXPERTS)
    ranked = jnp.arange(EXPERTS)
    quarter = EXPERTS // 4
    copies = jnp.where(ranked < quarter, 4, jnp.where(ranked < 2 * quarter, 2, 1))
    listing = jnp.repeat(ordering, copies, total_repeat_length=2 * EXPERTS)
    shuffle = jax.random.permutation(second_key, 2 * EXPERTS)
    return listing[shuffle].astype(jnp.int32)


def slot_weights(key, salt_value, row_count, col_count):
    holders = plan_of(key)
    weight_key = jax.random.fold_in(key, salt_value)
    spread = 1.0 / math.sqrt(row_count)

    def one_slot(expert):
        return jax.random.normal(jax.random.fold_in(weight_key, expert), (row_count, col_count), jnp.float32) * spread
    return jax.vmap(one_slot)(holders)


def draw_slot_expert(key, part):
    return plan_of(key)


def draw_gate_weight(key, part):
    return slot_weights(key, 21, D, HID).astype(jnp.bfloat16)


def draw_up_weight(key, part):
    return slot_weights(key, 22, D, HID).astype(jnp.bfloat16)


def draw_down_weight(key, part):
    return slot_weights(key, 23, HID, D).astype(jnp.bfloat16)


def steps_of(rng, extent, cuts, least, largest):
    gain, own = 1.0, jax.random.fold_in(rng, 6)
    for dim, blocks in cuts:
        heights = jnp.exp(jax.random.uniform(jax.random.fold_in(own, dim), (blocks,), jnp.float32, least / len(cuts), largest / len(cuts)))
        gain = gain * jnp.repeat(heights, extent[dim] // blocks).reshape([-1 if axis == dim else 1 for axis in range(len(extent))])
    return gain


def assign_block(own_key, own, number, rows, number_of, top, limit, skew):
    sequence = jax.random.permutation(own_key, number_of)
    packed, usual = load_shares(number_of, rows * top, limit, skew, True), load_shares(number_of, rows * top, limit, skew, False)
    places = jnp.arange(number_of)

    def named(tallies, rotation):
        used = int((tallies > 0).sum())
        fixed = max(1, used // 4)
        passed = fixed + (places - fixed + rotation * (used - fixed)) % max(1, number_of - fixed)
        return jnp.zeros((number_of,), jnp.int32).at[sequence[jnp.where(places < fixed, places, passed)]].set(jnp.asarray(tallies, jnp.int32))

    tallies = jnp.where(number % 4 == 0, named(packed, number // 4), named(usual, number - number // 4 - 1))
    mixed = jax.random.permutation(jax.random.fold_in(own, 3), number_of)
    giver, receiver = mixed[0:number_of // 2 * 2:2], mixed[1:number_of // 2 * 2:2]
    margin = jnp.minimum(tallies[giver] - 1, limit - tallies[receiver]) // 2
    margin = jnp.where((giver == sequence[0]) | (receiver == sequence[0]) | (tallies[receiver] == 0), 0, jnp.maximum(margin, 0))
    passed = jax.random.randint(jax.random.fold_in(own, 4), (number_of // 2,), 0, 1 << 20) % (margin + 1)
    tallies = tallies.at[giver].add(-passed).at[receiver].add(passed)
    items = jnp.searchsorted(jnp.cumsum(tallies), jnp.arange(rows * top), side="right").astype(jnp.int32)
    table = items.reshape(top, rows).T
    table = table[jax.random.permutation(jax.random.fold_in(own, 1), rows)]
    rotation = jax.random.randint(jax.random.fold_in(own, 2), (rows, 1), 0, top)
    return jnp.take_along_axis(table, (jnp.arange(top)[None, :] + rotation) % top, axis=1)


def load_shares(number_of, total, reach, skew, full):
    loads = [(1 << 20) // math.isqrt(grade ** skew) + 1 for grade in range(1, number_of + 1)]
    largest = reach if full else min(reach, max(-(-total // number_of), total * loads[0] // sum(loads)))
    least = 1 if total - largest >= number_of - 1 else 0
    counts, rest = [largest] + [least] * (number_of - 1), total - largest - least * (number_of - 1)
    while rest > 0:
        movable = [i for i in range(1, number_of) if counts[i] < largest] or [i for i in range(1, number_of) if counts[i] < reach]
        mass, budget = sum([loads[i] for i in movable]), rest
        for i in movable:
            addition = min(reach - counts[i], max(1, budget * loads[i] // mass), rest)
            counts[i] = counts[i] + addition
            rest = rest - addition
    return np.array(counts)


def scatter_about(key, dims, deviation, reach, pieces=(), held_as=jnp.bfloat16):
    drawn = jax.random.normal(key, dims, jnp.float32) * deviation
    if len(pieces) > 0:
        drawn = steps_of(key, dims, pieces, -0.22, 0.18) * drawn
    return jnp.clip(drawn, min=-reach, max=reach).astype(held_as)


def setup_inputs(seed: int = 0, part: int = 0) -> dict:
    seeds = jax.random.split(jax.random.key(seed), 8)
    own_keys = jax.random.split(jax.random.fold_in(seeds[7], part), 8)
    tokens = scatter_about(own_keys[0], (TOKENS, D), 1.0, 6.0, ((0, 8), (1, 2)))
    expert_ids_keys = jax.random.split(jax.random.fold_in(own_keys[1], 1), TOKENS // TOK_EP)
    expert_ids_turns = jax.random.permutation(jax.random.fold_in(own_keys[1], 3), TOKENS // TOK_EP)
    expert_ids = jax.vmap(lambda own, number: assign_block(jax.random.fold_in(own_keys[1], 2), own, number, TOK_EP, EXPERTS, TOP, CAP, 2))(expert_ids_keys, expert_ids_turns).reshape((TOKENS, TOP))
    gate_values = jnp.clip(0.1 + 0.5 * jax.random.uniform(own_keys[2], (TOKENS, TOP), jnp.float32) ** steps_of(own_keys[2], (TOKENS, TOP), ((0, 8),), -0.2, 0.2), 0.1, 0.6)
    slot_expert = draw_slot_expert(jax.random.fold_in(seeds[7], 71), part)
    gate_weight = draw_gate_weight(jax.random.fold_in(seeds[7], 71), part)
    up_weight = draw_up_weight(jax.random.fold_in(seeds[7], 71), part)
    down_weight = draw_down_weight(jax.random.fold_in(seeds[7], 71), part)
    return {"tokens": tokens, "expert_ids": expert_ids, "gate_values": gate_values, "slot_expert": slot_expert, "gate_weight": gate_weight, "up_weight": up_weight, "down_weight": down_weight}


def reference(tokens, expert_ids, gate_values, slot_expert, gate_weight, up_weight, down_weight):
    pair_count = TOKENS * TOP
    row_bound = min(pair_count, N_EP * CAP)
    pair_expert = expert_ids.reshape(pair_count)
    padded = jnp.concatenate([tokens, jnp.zeros((1, D), tokens.dtype)], axis=0)
    flat_gates = jnp.concatenate([gate_values.reshape(pair_count), jnp.zeros((1,), gate_values.dtype)], axis=0)

    def one_expert(running, expert):
        slot_index = jnp.argmax(slot_expert == expert).astype(jnp.int32)
        members = jnp.nonzero(pair_expert == expert, size=row_bound, fill_value=pair_count)[0].astype(jnp.int32)
        row_block = padded[members // TOP]
        gate_proj = jnp.dot(row_block, gate_weight[slot_index], preferred_element_type=jnp.float32)
        up_proj = jnp.dot(row_block, up_weight[slot_index], preferred_element_type=jnp.float32)
        hidden = (jax.nn.silu(gate_proj) * up_proj).astype(jnp.bfloat16)
        outcome = jnp.dot(hidden, down_weight[slot_index], preferred_element_type=jnp.float32).astype(jnp.bfloat16)
        weight = flat_gates[members]
        running = running.at[members // TOP].add(weight[:, None] * outcome.astype(jnp.float32))
        return running, None

    running, _ = lax.scan(one_expert, jnp.zeros((TOKENS + 1, D), jnp.float32), jnp.arange(EXPERTS, dtype=jnp.int32))
    return running[:TOKENS].astype(jnp.bfloat16)
```

```python
import functools

import jax
import jax.numpy as jnp
from jax import lax
from jax.experimental import pallas as pl
from jax.experimental.pallas import tpu as pltpu
from jax.sharding import PartitionSpec as P

LANES = 128
SUBLANES = 8
MIB = 1 << 20
F32 = jnp.float32
BF16 = jnp.bfloat16
TRANS_LHS = (((0,), (0,)), ((), ()))


class Plan:
    def __init__(self, tok, choices, feat, slots):
        experts = slots // 2
        self.tok, self.choices, self.feat, self.slots = tok, choices, feat, slots
        self.capacity = tok * choices * 5 // (4 * experts)
        assert feat % LANES == 0
        self.blocks = feat // LANES
        self.full = self.capacity // SUBLANES
        self.main = self.full * SUBLANES
        self.tail = self.capacity - self.main
        self.group = SUBLANES // self.tail if self.tail else 0
        self.tail_tiles = -(-self.blocks // self.group) if self.tail else 0
        self.tiles = self.full * self.blocks + self.tail_tiles
        self.main_rows = slots * self.main
        self.tail_rows = slots * self.tail
        self.rows = self.main_rows + self.tail_rows
        self.tail_wide = slots * SUBLANES if self.tail else 0
        self.wide = self.main_rows + self.tail_wide
        self.packed = (slots, self.tiles, SUBLANES, LANES)


def iota(shape, dim):
    return lax.broadcasted_iota(jnp.int32, shape, dim)


def floor_div(values, divisor):
    return jnp.floor((values.astype(F32) + 0.5) * (1.0 / divisor)).astype(jnp.int32)


def route(plan, member, slot_row, ids):
    slots, tok = plan.slots, plan.tok
    square = (slots, slots)
    down, across = iota(square, 0), iota(square, 1)
    row = jnp.broadcast_to(slot_row.astype(F32), square)
    col = jnp.sum(jnp.where(down == across, row, 0.0), axis=1, keepdims=True)
    same = jnp.where(col == row, 1.0, 0.0)
    copies = jnp.sum(same, axis=0, keepdims=True)
    rank = jnp.sum(jnp.where(down < across, same, 0.0), axis=0, keepdims=True)
    want = jnp.zeros((1, slots), F32)
    for number in (2, 3, 4):
        want = jnp.where(copies == number, lax.rem(member, number).astype(F32), want)
    chosen = rank == want
    hits = [
        jnp.where((ids[:, k : k + 1] == slot_row) & chosen, 1.0, 0.0) for k in range(plan.choices)
    ]
    before = jnp.where(iota((tok, tok), 1) < iota((tok, tok), 0), 1.0, 0.0).astype(BF16)
    counts = jnp.dot(before, sum(hits).astype(BF16), preferred_element_type=F32)
    lane = iota((tok, slots), 1).astype(F32)
    found = []
    for hit in hits:
        slot = jnp.sum(hit * lane, axis=1, keepdims=True).astype(jnp.int32)
        place = jnp.sum(hit * counts, axis=1, keepdims=True).astype(jnp.int32)
        found.append((slot, place))
    return found


def main_hot(plan, slot, place):
    code = jnp.where(place < plan.main, slot * plan.main + place, -1)
    return jnp.where(code == iota((plan.tok, plan.main_rows), 1), 1.0, 0.0)


def tail_hot(plan, slot, place, part):
    code = jnp.where(
        place < plan.main, -1, slot * SUBLANES + place - plan.main + part * plan.tail
    )
    return jnp.where(code == iota((plan.tok, plan.tail_wide), 1), 1.0, 0.0)


def lane_block(index):
    return slice(index * LANES, (index + 1) * LANES)


def pack_kernel(plan, member_ref, slot_ref, ids_ref, tokens_ref, send_ref):
    found = route(plan, member_ref[0], slot_ref[...], ids_ref[...])
    if plan.full:
        hot = sum(main_hot(plan, *pair) for pair in found).astype(BF16)
        main = lax.dot_general(hot, tokens_ref[...], TRANS_LHS, preferred_element_type=F32)
        for block in range(plan.blocks):
            tile = main[:, lane_block(block)].reshape(plan.slots, plan.full, SUBLANES, LANES)
            for index in range(plan.full):
                send_ref[:, index * plan.blocks + block] = tile[:, index].astype(BF16)
    if plan.tail:
        hot = jnp.concatenate(
            [sum(tail_hot(plan, *pair, part) for pair in found) for part in range(plan.group)],
            axis=0,
        ).astype(BF16)
        for index in range(plan.tail_tiles):
            stack = []
            for part in range(plan.group):
                block = index * plan.group + part
                if block < plan.blocks:
                    stack.append(tokens_ref[:, lane_block(block)])
                else:
                    stack.append(jnp.zeros((plan.tok, LANES), BF16))
            tile = lax.dot_general(
                hot, jnp.concatenate(stack, axis=0), TRANS_LHS, preferred_element_type=F32
            )
            send_ref[:, plan.full * plan.blocks + index] = tile.reshape(
                plan.slots, SUBLANES, LANES
            ).astype(BF16)


def flat_tile(tile):
    return tile.astype(F32).reshape(-1, LANES).astype(BF16)


def unpack_rows(plan, packed_ref, rows_ref):
    for block in range(plan.blocks):
        for index in range(plan.full):
            tile = packed_ref[:, index * plan.blocks + block]
            if plan.full == 1:
                rows_ref[0 : plan.main_rows, lane_block(block)] = flat_tile(tile)
            else:
                for sender in range(plan.slots):
                    first = sender * plan.main + index * SUBLANES
                    rows_ref[first : first + SUBLANES, lane_block(block)] = tile[sender]
    if plan.tail:
        shape = (plan.group * plan.tail_rows, plan.tail_wide)
        line = iota(shape, 0)
        part = floor_div(line, plan.tail_rows)
        inner = line - part * plan.tail_rows
        sender = floor_div(inner, plan.tail)
        spot = sender * SUBLANES + part * plan.tail + inner - sender * plan.tail
        hot = jnp.where(spot == iota(shape, 1), 1.0, 0.0).astype(BF16)
        for index in range(plan.tail_tiles):
            tile = flat_tile(packed_ref[:, plan.full * plan.blocks + index])
            moved = jnp.dot(hot, tile, preferred_element_type=F32).astype(BF16)
            for part in range(plan.group):
                block = index * plan.group + part
                if block < plan.blocks:
                    rows_ref[plan.main_rows : plan.rows, lane_block(block)] = moved[
                        part * plan.tail_rows : (part + 1) * plan.tail_rows
                    ]


def own_kernel(plan, core_ref, packed_ref, gate_ref, up_ref, acc_ref, rows_ref):
    unpack_rows(plan, packed_ref, rows_ref)
    first = pl.multiple_of(core_ref[0] * plan.feat, LANES)
    hid = gate_ref.shape[1]
    rows = rows_ref[...]
    acc_ref[:, :hid] = jnp.dot(
        rows, gate_ref[pl.ds(first, plan.feat), :], preferred_element_type=F32
    )
    acc_ref[:, hid:] = jnp.dot(
        rows, up_ref[pl.ds(first, plan.feat), :], preferred_element_type=F32
    )


def emit_packed(plan, product, out_ref):
    for block in range(plan.blocks):
        tile = product[: plan.main_rows, lane_block(block)].reshape(
            plan.slots, plan.full, SUBLANES, LANES
        )
        for index in range(plan.full):
            out_ref[:, index * plan.blocks + block] = tile[:, index].astype(out_ref.dtype)
    for index in range(plan.tail_tiles):
        spot = iota((plan.tail_wide, LANES), 0)
        spot = spot - floor_div(spot, SUBLANES) * SUBLANES
        tile = jnp.zeros((plan.tail_wide, LANES), F32)
        for part in range(plan.group):
            block = index * plan.group + part
            if block < plan.blocks:
                here = (spot >= part * plan.tail) & (spot < (part + 1) * plan.tail)
                tile = jnp.where(here, product[plan.main_rows :, lane_block(block)], tile)
        out_ref[:, plan.full * plan.blocks + index] = tile.reshape(
            plan.slots, SUBLANES, LANES
        ).astype(out_ref.dtype)


def other_kernel(
    plan, core_ref, packed_ref, acc_ref, gate_ref, up_ref, down_ref, hidden_ref, out_ref, rows_ref
):
    unpack_rows(plan, packed_ref, rows_ref)
    first = pl.multiple_of((1 - core_ref[0]) * plan.feat, LANES)
    hid = gate_ref.shape[1]
    rows = rows_ref[...]
    gate = acc_ref[:, :hid] + jnp.dot(
        rows, gate_ref[pl.ds(first, plan.feat), :], preferred_element_type=F32
    )
    up = acc_ref[:, hid:] + jnp.dot(
        rows, up_ref[pl.ds(first, plan.feat), :], preferred_element_type=F32
    )
    hidden = (gate / (1.0 + jnp.exp(-gate)) * up).astype(BF16)
    if plan.full:
        hidden_ref[: plan.main_rows] = hidden[: plan.main_rows]
    if plan.tail:
        shape = (plan.tail_wide, plan.tail_rows)
        line, col = iota(shape, 0), iota(shape, 1)
        sender = floor_div(line, SUBLANES)
        spot = line - sender * SUBLANES
        spot = spot - floor_div(spot, plan.tail) * plan.tail
        hot = jnp.where(sender * plan.tail + spot == col, 1.0, 0.0).astype(BF16)
        hidden_ref[plan.main_rows :] = jnp.dot(
            hot, hidden[plan.main_rows :], preferred_element_type=F32
        ).astype(BF16)
    product = jnp.dot(
        hidden_ref[...], down_ref[:, pl.ds(first, plan.feat)], preferred_element_type=F32
    )
    emit_packed(plan, product, out_ref)


def down_kernel(plan, core_ref, hidden_ref, down_ref, out_ref):
    first = pl.multiple_of(core_ref[0] * plan.feat, LANES)
    product = jnp.dot(
        hidden_ref[...], down_ref[:, pl.ds(first, plan.feat)], preferred_element_type=F32
    )
    emit_packed(plan, product, out_ref)


def combine_kernel(plan, member_ref, slot_ref, ids_ref, gates_ref, packed_ref, out_ref):
    found = route(plan, member_ref[0], slot_ref[...], ids_ref[...])
    hots = []
    for slot, place in found:
        main = [main_hot(plan, slot, place)] if plan.full else []
        parts = range(plan.group) if plan.tail else range(1)
        hots.append(
            [
                jnp.concatenate(
                    main + ([tail_hot(plan, slot, place, part)] if plan.tail else []), axis=1
                ).astype(BF16)
                for part in parts
            ]
        )
    for block in range(plan.blocks):
        stack = []
        if plan.full == 1:
            stack.append(packed_ref[:, block].astype(F32).reshape(plan.main_rows, LANES))
        elif plan.full:
            tiles = [
                packed_ref[:, index * plan.blocks + block].astype(F32)[:, None]
                for index in range(plan.full)
            ]
            stack.append(jnp.concatenate(tiles, axis=1).reshape(plan.main_rows, LANES))
        part = 0
        if plan.tail:
            index, part = divmod(block, plan.group)
            tile = packed_ref[:, plan.full * plan.blocks + index]
            stack.append(tile.astype(F32).reshape(plan.tail_wide, LANES))
        table = jnp.concatenate(stack, axis=0).astype(BF16)
        total = jnp.zeros((plan.tok, LANES), F32)
        for k in range(plan.choices):
            picked = jnp.dot(hots[k][part], table, preferred_element_type=F32)
            total = total + gates_ref[:, k : k + 1] * picked
        out_ref[:, lane_block(block)] = total.astype(BF16)


SMEM = pl.BlockSpec(memory_space=pltpu.SMEM)
VMEM = pl.BlockSpec(memory_space=pltpu.VMEM)


def call(kernel, name, in_specs, out_shape, flops, moved, limit, scratch=()):
    single = not isinstance(out_shape, (list, tuple))
    return pl.pallas_call(
        kernel,
        name=name,
        in_specs=in_specs,
        out_specs=VMEM if single else [VMEM] * len(out_shape),
        out_shape=out_shape,
        scratch_shapes=list(scratch),
        cost_estimate=pl.CostEstimate(flops=flops, bytes_accessed=moved, transcendentals=0),
        compiler_params=pltpu.CompilerParams(vmem_limit_bytes=limit),
    )


def body(tokens, expert_ids, gate_values, slot_expert, gate_weight, up_weight, down_weight):
    tok, choices = expert_ids.shape
    feat = tokens.shape[1]
    slots = slot_expert.shape[0]
    plan = Plan(tok, choices, feat, slots)
    gate_local, up_local, down_local = gate_weight[0], up_weight[0], down_weight[0]
    hid = gate_local.shape[1]
    member = lax.axis_index("ep").astype(jnp.int32).reshape(1)
    core = lax.axis_index("rep").astype(jnp.int32).reshape(1)
    slot_row = slot_expert.reshape(1, slots)
    swap = [(0, 1), (1, 0)]
    packed_bytes = 2 * slots * plan.tiles * SUBLANES * LANES
    half_flops = 4 * plan.rows * feat * hid
    rows_scratch = pltpu.VMEM((plan.rows, feat), BF16)

    send = call(
        functools.partial(pack_kernel, plan),
        "pack",
        [SMEM, VMEM, VMEM, VMEM],
        jax.ShapeDtypeStruct(plan.packed, BF16),
        4 * tok * feat * plan.wide,
        2 * packed_bytes,
        16 * MIB,
    )(member, slot_row, expert_ids, tokens)
    arrived = lax.all_to_all(send, "ep", split_axis=0, concat_axis=0, tiled=True)
    partner = lax.ppermute(arrived, "rep", swap)
    acc = call(
        functools.partial(own_kernel, plan),
        "own_half",
        [SMEM, VMEM, VMEM, VMEM],
        jax.ShapeDtypeStruct((plan.rows, 2 * hid), F32),
        half_flops,
        packed_bytes + 8 * plan.rows * hid,
        24 * MIB,
        [rows_scratch],
    )(core, arrived, gate_local, up_local)
    hidden, outbound = call(
        functools.partial(other_kernel, plan),
        "other_half",
        [SMEM, VMEM, VMEM, VMEM, VMEM, VMEM],
        [
            jax.ShapeDtypeStruct((plan.wide, hid), BF16),
            jax.ShapeDtypeStruct(plan.packed, BF16),
        ],
        half_flops + 2 * plan.wide * hid * feat,
        2 * packed_bytes + 8 * plan.rows * hid,
        24 * MIB,
        [rows_scratch],
    )(core, partner, acc, gate_local, up_local, down_local)
    received = lax.ppermute(outbound, "rep", swap)
    mine = call(
        functools.partial(down_kernel, plan),
        "down_own",
        [SMEM, VMEM, VMEM],
        jax.ShapeDtypeStruct(plan.packed, F32),
        2 * plan.wide * hid * feat,
        2 * packed_bytes,
        16 * MIB,
    )(core, hidden, down_local)
    result = (mine + received.astype(F32)).astype(BF16)
    returned = lax.all_to_all(result, "ep", split_axis=0, concat_axis=0, tiled=True)
    return call(
        functools.partial(combine_kernel, plan),
        "combine",
        [SMEM, VMEM, VMEM, VMEM, VMEM],
        jax.ShapeDtypeStruct((tok, feat), BF16),
        2 * tok * feat * plan.wide * choices,
        2 * packed_bytes,
        16 * MIB,
    )(member, slot_row, expert_ids, gate_values, returned)


def solution(mesh):
    assert mesh.shape["rep"] == 2
    return jax.shard_map(
        body,
        mesh=mesh,
        in_specs=(
            P(("groups", "ep"), "rep"),
            P(("groups", "ep"), None),
            P(("groups", "ep"), None),
            P(),
            P("ep", None, "rep"),
            P("ep", None, "rep"),
            P("ep", "rep", None),
        ),
        out_specs=P(("groups", "ep"), "rep"),
        check_vma=False,
    )
```

```python
import functools

import jax
import jax.numpy as jnp
from jax import lax
from jax.experimental import pallas as pl
from jax.experimental.pallas import tpu as pltpu
from jax.sharding import PartitionSpec as P


LANES = 128
SUBLANES = 8
MIB = 1 << 20
F32 = jnp.float32
BF16 = jnp.bfloat16
COVER_FLOPS = 1 << 34
COVER_BYTES = 1 << 25


class Plan:
    def __init__(self, tok, choices, feat, slots):
        experts = slots // 2
        self.tok, self.choices, self.feat, self.slots = tok, choices, feat, slots
        self.capacity = tok * choices * 5 // (4 * experts)
        assert feat % LANES == 0
        self.blocks = feat // LANES
        self.full = self.capacity // SUBLANES
        self.main = self.full * SUBLANES
        self.tail = self.capacity - self.main
        self.group = SUBLANES // self.tail if self.tail else 0
        self.tail_tiles = -(-self.blocks // self.group) if self.tail else 0
        self.tiles = self.full * self.blocks + self.tail_tiles
        self.main_rows = slots * self.main
        self.tail_rows = slots * self.tail
        self.rows = self.main_rows + self.tail_rows
        self.tail_wide = slots * SUBLANES if self.tail else 0
        self.wide = self.main_rows + self.tail_wide
        self.parts = max(1, self.group)
        self.packed = (slots, self.tiles, SUBLANES, LANES)


def iota(shape, dim):
    return lax.broadcasted_iota(jnp.int32, shape, dim)


def floor_div(values, divisor):
    return jnp.floor((values.astype(F32) + 0.5) * (1.0 / divisor)).astype(jnp.int32)


def to_column(row):
    size = row.shape[1]
    diagonal = iota((size, size), 0) == iota((size, size), 1)
    return jnp.sum(jnp.where(diagonal, jnp.broadcast_to(row, (size, size)), 0), axis=1, keepdims=True)


def route(plan, member, slot_row, ids):
    slots, tok = plan.slots, plan.tok
    square = (slots, slots)
    row = slot_row.astype(F32)
    col = to_column(row)
    same = jnp.where(col == row, 1.0, 0.0)
    copies = jnp.sum(same, axis=1, keepdims=True)
    rank = jnp.sum(jnp.where(iota(square, 1) < iota(square, 0), same, 0.0), axis=1, keepdims=True)
    want = jnp.zeros((slots, 1), F32)
    for number in (2, 3, 4):
        want = jnp.where(copies == number, lax.rem(member, number).astype(F32), want)
    chosen = rank == want
    hits = [
        jnp.where((ids[k : k + 1].astype(F32) == col) & chosen, 1.0, 0.0)
        for k in range(plan.choices)
    ]
    before = jnp.where(iota((tok, tok), 0) < iota((tok, tok), 1), 1.0, 0.0).astype(BF16)
    counts = jnp.dot(sum(hits).astype(BF16), before, preferred_element_type=F32)
    line = iota((slots, tok), 0).astype(F32)
    found = []
    for hit in hits:
        slot = jnp.sum(hit * line, axis=0, keepdims=True).astype(jnp.int32)
        place = jnp.sum(hit * counts, axis=0, keepdims=True).astype(jnp.int32)
        found.append((slot, place))
    return found


def main_code(plan, slot, place):
    return jnp.where(place < plan.main, slot * plan.main + place, -1)


def tail_code(plan, slot, place, part):
    spot = slot * SUBLANES + place - plan.main + part * plan.tail
    return jnp.where(place < plan.main, -1, spot)


def lane_block(index):
    return slice(index * LANES, (index + 1) * LANES)


def warm_kernel(out_ref):
    out_ref[...] = jnp.zeros_like(out_ref)


def read_found(plan, found_ref):
    lines = [found_ref[index : index + 1] for index in range(2 * plan.choices)]
    return list(zip(lines[: plan.choices], lines[plan.choices :], strict=True))


def pack_kernel(plan, warm_ref, slot_ref, ids_ref, tokens_ref, send_ref, found_ref):
    found = route(plan, lax.axis_index("ep"), slot_ref[...], ids_ref[...])
    for k, (slot, place) in enumerate(found):
        found_ref[k : k + 1] = slot
        found_ref[plan.choices + k : plan.choices + k + 1] = place
    if plan.full:
        line = iota((plan.main_rows, plan.tok), 0)
        hot = sum(jnp.where(line == main_code(plan, *pair), 1.0, 0.0) for pair in found)
        main = jnp.dot(hot.astype(BF16), tokens_ref[...], preferred_element_type=F32)
        for block in range(plan.blocks):
            tile = main[:, lane_block(block)].reshape(plan.slots, plan.full, SUBLANES, LANES)
            for index in range(plan.full):
                send_ref[:, index * plan.blocks + block] = tile[:, index].astype(BF16)
    if plan.tail:
        line = iota((plan.tail_wide, plan.tok * plan.group), 0)
        hot = jnp.zeros(line.shape, F32)
        for pair in found:
            codes = [tail_code(plan, *pair, part) for part in range(plan.group)]
            hot += jnp.where(line == jnp.concatenate(codes, axis=1), 1.0, 0.0)
        hot = hot.astype(BF16)
        for index in range(plan.tail_tiles):
            stack = []
            for part in range(plan.group):
                block = index * plan.group + part
                if block < plan.blocks:
                    stack.append(tokens_ref[:, lane_block(block)])
                else:
                    stack.append(jnp.zeros((plan.tok, LANES), BF16))
            tile = jnp.dot(hot, jnp.concatenate(stack, axis=0), preferred_element_type=F32)
            send_ref[:, plan.full * plan.blocks + index] = tile.reshape(
                plan.slots, SUBLANES, LANES
            ).astype(BF16)


def select_kernel(plan, found_ref, gates_ref, pick_ref, column_ref):
    lane = iota((plan.tok, plan.wide), 1).astype(F32)
    for k, (slot, place) in enumerate(read_found(plan, found_ref)):
        column_ref[:, k : k + 1] = to_column(gates_ref[k : k + 1])
        for part in range(plan.parts):
            tail = plan.main_rows + tail_code(plan, slot, place, part)
            code = jnp.where(place < plan.main, main_code(plan, slot, place), tail)
            pick = jnp.where(to_column(code.astype(F32)) == lane, 1.0, 0.0)
            pick_ref[k * plan.parts + part] = pick.astype(BF16)


def flat_tile(tile):
    return tile.astype(F32).reshape(-1, LANES).astype(BF16)


def unpack_rows(plan, packed_ref, rows_ref):
    for block in range(plan.blocks):
        for index in range(plan.full):
            tile = packed_ref[:, index * plan.blocks + block]
            if plan.full == 1:
                rows_ref[0 : plan.main_rows, lane_block(block)] = flat_tile(tile)
            else:
                for sender in range(plan.slots):
                    first = sender * plan.main + index * SUBLANES
                    rows_ref[first : first + SUBLANES, lane_block(block)] = tile[sender]
    if plan.tail:
        shape = (plan.group * plan.tail_rows, plan.tail_wide)
        line = iota(shape, 0)
        part = floor_div(line, plan.tail_rows)
        inner = line - part * plan.tail_rows
        sender = floor_div(inner, plan.tail)
        spot = sender * SUBLANES + part * plan.tail + inner - sender * plan.tail
        hot = jnp.where(spot == iota(shape, 1), 1.0, 0.0).astype(BF16)
        for index in range(plan.tail_tiles):
            tile = flat_tile(packed_ref[:, plan.full * plan.blocks + index])
            moved = jnp.dot(hot, tile, preferred_element_type=F32).astype(BF16)
            for part in range(plan.group):
                block = index * plan.group + part
                if block < plan.blocks:
                    rows_ref[plan.main_rows : plan.rows, lane_block(block)] = moved[
                        part * plan.tail_rows : (part + 1) * plan.tail_rows
                    ]


def own_kernel(plan, packed_ref, gate_ref, up_ref, down_ref, acc_ref, rows_ref):
    unpack_rows(plan, packed_ref, rows_ref)
    first = pl.multiple_of(lax.axis_index("rep") * plan.feat, LANES)
    hid = gate_ref.shape[1]
    rows = rows_ref[...]
    acc_ref[:, :hid] = jnp.dot(
        rows, gate_ref[pl.ds(first, plan.feat), :], preferred_element_type=F32
    )
    acc_ref[:, hid:] = jnp.dot(
        rows, up_ref[pl.ds(first, plan.feat), :], preferred_element_type=F32
    )


def emit_packed(plan, product, out_ref):
    for block in range(plan.blocks):
        tile = product[: plan.main_rows, lane_block(block)].reshape(
            plan.slots, plan.full, SUBLANES, LANES
        )
        for index in range(plan.full):
            out_ref[:, index * plan.blocks + block] = tile[:, index].astype(out_ref.dtype)
    for index in range(plan.tail_tiles):
        spot = iota((plan.tail_wide, LANES), 0)
        spot = spot - floor_div(spot, SUBLANES) * SUBLANES
        tile = jnp.zeros((plan.tail_wide, LANES), F32)
        for part in range(plan.group):
            block = index * plan.group + part
            if block < plan.blocks:
                here = (spot >= part * plan.tail) & (spot < (part + 1) * plan.tail)
                tile = jnp.where(here, product[plan.main_rows :, lane_block(block)], tile)
        out_ref[:, plan.full * plan.blocks + index] = tile.reshape(
            plan.slots, SUBLANES, LANES
        ).astype(out_ref.dtype)


def other_kernel(
    plan, packed_ref, acc_ref, gate_ref, up_ref, down_ref, hidden_ref, out_ref, rows_ref
):
    unpack_rows(plan, packed_ref, rows_ref)
    first = pl.multiple_of((1 - lax.axis_index("rep")) * plan.feat, LANES)
    hid = gate_ref.shape[1]
    rows = rows_ref[...]
    gate = acc_ref[:, :hid] + jnp.dot(
        rows, gate_ref[pl.ds(first, plan.feat), :], preferred_element_type=F32
    )
    up = acc_ref[:, hid:] + jnp.dot(
        rows, up_ref[pl.ds(first, plan.feat), :], preferred_element_type=F32
    )
    hidden = (gate / (1.0 + jnp.exp(-gate)) * up).astype(BF16)
    if plan.full:
        hidden_ref[: plan.main_rows] = hidden[: plan.main_rows]
    if plan.tail:
        shape = (plan.tail_wide, plan.tail_rows)
        line, col = iota(shape, 0), iota(shape, 1)
        sender = floor_div(line, SUBLANES)
        spot = line - sender * SUBLANES
        spot = spot - floor_div(spot, plan.tail) * plan.tail
        hot = jnp.where(sender * plan.tail + spot == col, 1.0, 0.0).astype(BF16)
        hidden_ref[plan.main_rows :] = jnp.dot(
            hot, hidden[plan.main_rows :], preferred_element_type=F32
        ).astype(BF16)
    product = jnp.dot(
        hidden_ref[...], down_ref[:, pl.ds(first, plan.feat)], preferred_element_type=F32
    )
    emit_packed(plan, product, out_ref)


def down_kernel(plan, hidden_ref, down_ref, out_ref):
    first = pl.multiple_of(lax.axis_index("rep") * plan.feat, LANES)
    product = jnp.dot(
        hidden_ref[...], down_ref[:, pl.ds(first, plan.feat)], preferred_element_type=F32
    )
    emit_packed(plan, product, out_ref)


def sum_kernel(mine_ref, other_ref, out_ref):
    out_ref[...] = (mine_ref[...] + other_ref[...].astype(F32)).astype(BF16)


def combine_kernel(plan, pick_ref, column_ref, packed_ref, out_ref):
    for block in range(plan.blocks):
        stack = []
        if plan.full == 1:
            stack.append(packed_ref[:, block].astype(F32).reshape(plan.main_rows, LANES))
        elif plan.full:
            tiles = [
                packed_ref[:, index * plan.blocks + block].astype(F32)[:, None]
                for index in range(plan.full)
            ]
            stack.append(jnp.concatenate(tiles, axis=1).reshape(plan.main_rows, LANES))
        part = 0
        if plan.tail:
            index, part = divmod(block, plan.group)
            tile = packed_ref[:, plan.full * plan.blocks + index]
            stack.append(tile.astype(F32).reshape(plan.tail_wide, LANES))
        table = jnp.concatenate(stack, axis=0).astype(BF16)
        total = jnp.zeros((plan.tok, LANES), F32)
        for k in range(plan.choices):
            picked = jnp.dot(
                pick_ref[k * plan.parts + part], table, preferred_element_type=F32
            )
            total = total + column_ref[:, k : k + 1] * picked
        out_ref[:, lane_block(block)] = total.astype(BF16)


VMEM = pl.BlockSpec(memory_space=pltpu.VMEM)
ANY = pl.BlockSpec(memory_space=pltpu.HBM)


def call(kernel, in_specs, out_shape, flops, moved, limit, scratch=()):
    single = not isinstance(out_shape, (list, tuple))
    return pl.pallas_call(
        kernel,
        in_specs=in_specs,
        out_specs=VMEM if single else [VMEM] * len(out_shape),
        out_shape=out_shape,
        scratch_shapes=list(scratch),
        cost_estimate=pl.CostEstimate(flops=flops, bytes_accessed=moved, transcendentals=0),
        compiler_params=pltpu.CompilerParams(vmem_limit_bytes=limit),
    )


def body(tokens, expert_ids, gate_values, slot_expert, gate_weight, up_weight, down_weight):
    tok, choices = expert_ids.shape
    feat = tokens.shape[1]
    slots = slot_expert.shape[0]
    plan = Plan(tok, choices, feat, slots)
    weights = [gate_weight[0], up_weight[0], down_weight[0]]
    hid = weights[0].shape[1]
    gate_local, up_local, down_local = weights
    swap = [(0, 1), (1, 0)]
    packed_bytes = 2 * slots * plan.tiles * SUBLANES * LANES
    half_flops = 4 * plan.rows * feat * hid
    rows_scratch = pltpu.VMEM((plan.rows, feat), BF16)
    packed = jax.ShapeDtypeStruct(plan.packed, BF16)

    slot_row, ids, gates = slot_expert.reshape(1, slots), expert_ids.T, gate_values.T

    warm = call(
        warm_kernel,
        [],
        jax.ShapeDtypeStruct((SUBLANES, LANES), F32),
        COVER_FLOPS,
        COVER_BYTES,
        1 * MIB,
    )()
    send, found = call(
        functools.partial(pack_kernel, plan),
        [VMEM] * 4,
        [packed, jax.ShapeDtypeStruct((2 * choices, tok), jnp.int32)],
        COVER_FLOPS,
        COVER_BYTES,
        8 * MIB,
    )(warm, slot_row, ids, tokens)
    arrived = lax.all_to_all(send, "ep", split_axis=0, concat_axis=0, tiled=True)
    partner = lax.ppermute(arrived, "rep", swap)
    acc = call(
        functools.partial(own_kernel, plan),
        [VMEM] * 4,
        jax.ShapeDtypeStruct((plan.rows, 2 * hid), F32),
        1 << 10,
        1 << 10,
        8 * MIB,
        [rows_scratch],
    )(arrived, gate_local, up_local, down_local)
    picks, columns = call(
        functools.partial(select_kernel, plan),
        [VMEM, VMEM],
        [
            jax.ShapeDtypeStruct((choices * plan.parts, tok, plan.wide), BF16),
            jax.ShapeDtypeStruct((tok, choices), F32),
        ],
        1 << 10,
        1 << 10,
        4 * MIB,
    )(found, gates)
    hidden, outbound = call(
        functools.partial(other_kernel, plan),
        [VMEM, VMEM, VMEM, VMEM, VMEM],
        [jax.ShapeDtypeStruct((plan.wide, hid), BF16), packed],
        half_flops + 2 * plan.wide * hid * feat,
        2 * packed_bytes + 8 * plan.rows * hid,
        8 * MIB,
        [rows_scratch],
    )(partner, acc, gate_local, up_local, down_local)
    received = lax.ppermute(outbound, "rep", swap)
    mine = call(
        functools.partial(down_kernel, plan),
        [VMEM, VMEM],
        jax.ShapeDtypeStruct(plan.packed, F32),
        2 * plan.wide * hid * feat,
        2 * packed_bytes,
        8 * MIB,
    )(hidden, down_local)
    result = call(
        sum_kernel, [VMEM, VMEM], packed, packed_bytes, 4 * packed_bytes, 4 * MIB
    )(mine, received)
    returned = lax.all_to_all(result, "ep", split_axis=0, concat_axis=0, tiled=True)
    return call(
        functools.partial(combine_kernel, plan),
        [VMEM, VMEM, VMEM],
        jax.ShapeDtypeStruct((tok, feat), BF16),
        2 * tok * feat * plan.wide * choices,
        2 * packed_bytes,
        8 * MIB,
    )(picks, columns, returned)


def solution(mesh):
    assert mesh.shape["rep"] == 2
    return jax.shard_map(
        body,
        mesh=mesh,
        in_specs=(
            P(("groups", "ep"), "rep"),
            P(("groups", "ep"), None),
            P(("groups", "ep"), None),
            P(),
            P("ep", None, "rep"),
            P("ep", None, "rep"),
            P("ep", "rep", None),
        ),
        out_specs=P(("groups", "ep"), "rep"),
        check_vma=False,
    )
```

```python
import functools

import jax
import jax.numpy as jnp
from jax import lax
from jax.experimental import pallas as pl
from jax.experimental.pallas import tpu as pltpu
from jax.sharding import PartitionSpec as P


LANES = 128
SUBLANES = 8
MIB = 1 << 20
F32 = jnp.float32
BF16 = jnp.bfloat16
COVER_FLOPS = 1 << 34
COVER_BYTES = 1 << 25


class Plan:
    def __init__(self, tok, choices, feat, slots):
        experts = slots // 2
        self.tok, self.choices, self.feat, self.slots = tok, choices, feat, slots
        self.capacity = tok * choices * 5 // (4 * experts)
        assert feat % LANES == 0
        self.blocks = feat // LANES
        self.full = self.capacity // SUBLANES
        self.main = self.full * SUBLANES
        self.tail = self.capacity - self.main
        self.group = SUBLANES // self.tail if self.tail else 0
        self.tail_tiles = -(-self.blocks // self.group) if self.tail else 0
        self.tiles = self.full * self.blocks + self.tail_tiles
        self.main_rows = slots * self.main
        self.tail_rows = slots * self.tail
        self.rows = self.main_rows + self.tail_rows
        self.tail_wide = slots * SUBLANES if self.tail else 0
        self.wide = self.main_rows + self.tail_wide
        self.parts = max(1, self.group)
        self.packed = (slots, self.tiles, SUBLANES, LANES)


def iota(shape, dim):
    return lax.broadcasted_iota(jnp.int32, shape, dim)


def floor_div(values, divisor):
    return jnp.floor((values.astype(F32) + 0.5) * (1.0 / divisor)).astype(jnp.int32)


def exchange_order(members):
    return sorted(range(members), key=lambda index: exchange_place(index, members))


def exchange_place(index, members):
    away = index - members // 2
    return 2 * away if away >= 0 else -2 * away - 1


def exchange(array, members):
    return lax.all_to_all(
        array,
        "ep",
        split_axis=0,
        concat_axis=0,
        tiled=True,
        axis_index_groups=[exchange_order(members)],
    )


def to_column(row):
    size = row.shape[1]
    diagonal = iota((size, size), 0) == iota((size, size), 1)
    return jnp.sum(jnp.where(diagonal, jnp.broadcast_to(row, (size, size)), 0), axis=1, keepdims=True)


def route(plan, member, slot_row, ids):
    slots, tok = plan.slots, plan.tok
    square = (slots, slots)
    row = slot_row.astype(F32)
    col = to_column(row)
    same = jnp.where(col == row, 1.0, 0.0)
    copies = jnp.sum(same, axis=1, keepdims=True)
    rank = jnp.sum(jnp.where(iota(square, 1) < iota(square, 0), same, 0.0), axis=1, keepdims=True)
    want = jnp.zeros((slots, 1), F32)
    for number in (2, 3, 4):
        want = jnp.where(copies == number, lax.rem(member, number).astype(F32), want)
    chosen = rank == want
    hits = [
        jnp.where((ids[k : k + 1].astype(F32) == col) & chosen, 1.0, 0.0)
        for k in range(plan.choices)
    ]
    before = jnp.where(iota((tok, tok), 0) < iota((tok, tok), 1), 1.0, 0.0).astype(BF16)
    counts = jnp.dot(sum(hits).astype(BF16), before, preferred_element_type=F32)
    away = iota((slots, tok), 0) - slots // 2
    line = jnp.where(away >= 0, 2 * away, -2 * away - 1).astype(F32)
    found = []
    for hit in hits:
        slot = jnp.sum(hit * line, axis=0, keepdims=True).astype(jnp.int32)
        place = jnp.sum(hit * counts, axis=0, keepdims=True).astype(jnp.int32)
        found.append((slot, place))
    return found


def main_code(plan, slot, place):
    return jnp.where(place < plan.main, slot * plan.main + place, -1)


def tail_code(plan, slot, place, part):
    spot = slot * SUBLANES + place - plan.main + part * plan.tail
    return jnp.where(place < plan.main, -1, spot)


def lane_block(index):
    return slice(index * LANES, (index + 1) * LANES)


def warm_kernel(out_ref):
    out_ref[...] = jnp.zeros_like(out_ref)


def read_found(plan, found_ref):
    lines = [found_ref[index : index + 1] for index in range(2 * plan.choices)]
    return list(zip(lines[: plan.choices], lines[plan.choices :], strict=True))


def pack_kernel(plan, warm_ref, slot_ref, ids_ref, tokens_ref, send_ref, found_ref):
    found = route(plan, lax.axis_index("ep"), slot_ref[...], ids_ref[...])
    for k, (slot, place) in enumerate(found):
        found_ref[k : k + 1] = slot
        found_ref[plan.choices + k : plan.choices + k + 1] = place
    if plan.full:
        line = iota((plan.main_rows, plan.tok), 0)
        hot = sum(jnp.where(line == main_code(plan, *pair), 1.0, 0.0) for pair in found)
        main = jnp.dot(hot.astype(BF16), tokens_ref[...], preferred_element_type=F32)
        for block in range(plan.blocks):
            tile = main[:, lane_block(block)].reshape(plan.slots, plan.full, SUBLANES, LANES)
            for index in range(plan.full):
                send_ref[:, index * plan.blocks + block] = tile[:, index].astype(BF16)
    if plan.tail:
        line = iota((plan.tail_wide, plan.tok * plan.group), 0)
        hot = jnp.zeros(line.shape, F32)
        for pair in found:
            codes = [tail_code(plan, *pair, part) for part in range(plan.group)]
            hot += jnp.where(line == jnp.concatenate(codes, axis=1), 1.0, 0.0)
        hot = hot.astype(BF16)
        for index in range(plan.tail_tiles):
            stack = []
            for part in range(plan.group):
                block = index * plan.group + part
                if block < plan.blocks:
                    stack.append(tokens_ref[:, lane_block(block)])
                else:
                    stack.append(jnp.zeros((plan.tok, LANES), BF16))
            tile = jnp.dot(hot, jnp.concatenate(stack, axis=0), preferred_element_type=F32)
            send_ref[:, plan.full * plan.blocks + index] = tile.reshape(
                plan.slots, SUBLANES, LANES
            ).astype(BF16)


def select_kernel(plan, found_ref, gates_ref, pick_ref, column_ref):
    lane = iota((plan.tok, plan.wide), 1).astype(F32)
    for k, (slot, place) in enumerate(read_found(plan, found_ref)):
        column_ref[:, k : k + 1] = to_column(gates_ref[k : k + 1])
        for part in range(plan.parts):
            tail = plan.main_rows + tail_code(plan, slot, place, part)
            code = jnp.where(place < plan.main, main_code(plan, slot, place), tail)
            pick = jnp.where(to_column(code.astype(F32)) == lane, 1.0, 0.0)
            pick_ref[k * plan.parts + part] = pick.astype(BF16)


def flat_tile(tile):
    return tile.astype(F32).reshape(-1, LANES).astype(BF16)


def unpack_rows(plan, packed_ref, rows_ref):
    for block in range(plan.blocks):
        for index in range(plan.full):
            tile = packed_ref[:, index * plan.blocks + block]
            if plan.full == 1:
                rows_ref[0 : plan.main_rows, lane_block(block)] = flat_tile(tile)
            else:
                for sender in range(plan.slots):
                    first = sender * plan.main + index * SUBLANES
                    rows_ref[first : first + SUBLANES, lane_block(block)] = tile[sender]
    if plan.tail:
        shape = (plan.group * plan.tail_rows, plan.tail_wide)
        line = iota(shape, 0)
        part = floor_div(line, plan.tail_rows)
        inner = line - part * plan.tail_rows
        sender = floor_div(inner, plan.tail)
        spot = sender * SUBLANES + part * plan.tail + inner - sender * plan.tail
        hot = jnp.where(spot == iota(shape, 1), 1.0, 0.0).astype(BF16)
        for index in range(plan.tail_tiles):
            tile = flat_tile(packed_ref[:, plan.full * plan.blocks + index])
            moved = jnp.dot(hot, tile, preferred_element_type=F32).astype(BF16)
            for part in range(plan.group):
                block = index * plan.group + part
                if block < plan.blocks:
                    rows_ref[plan.main_rows : plan.rows, lane_block(block)] = moved[
                        part * plan.tail_rows : (part + 1) * plan.tail_rows
                    ]


def own_kernel(plan, packed_ref, gate_ref, up_ref, down_ref, acc_ref, rows_ref):
    unpack_rows(plan, packed_ref, rows_ref)
    first = pl.multiple_of(lax.axis_index("rep") * plan.feat, LANES)
    hid = gate_ref.shape[1]
    rows = rows_ref[...]
    acc_ref[:, :hid] = jnp.dot(
        rows, gate_ref[pl.ds(first, plan.feat), :], preferred_element_type=F32
    )
    acc_ref[:, hid:] = jnp.dot(
        rows, up_ref[pl.ds(first, plan.feat), :], preferred_element_type=F32
    )


def emit_packed(plan, product, out_ref):
    for block in range(plan.blocks):
        tile = product[: plan.main_rows, lane_block(block)].reshape(
            plan.slots, plan.full, SUBLANES, LANES
        )
        for index in range(plan.full):
            out_ref[:, index * plan.blocks + block] = tile[:, index].astype(out_ref.dtype)
    for index in range(plan.tail_tiles):
        spot = iota((plan.tail_wide, LANES), 0)
        spot = spot - floor_div(spot, SUBLANES) * SUBLANES
        tile = jnp.zeros((plan.tail_wide, LANES), F32)
        for part in range(plan.group):
            block = index * plan.group + part
            if block < plan.blocks:
                here = (spot >= part * plan.tail) & (spot < (part + 1) * plan.tail)
                tile = jnp.where(here, product[plan.main_rows :, lane_block(block)], tile)
        out_ref[:, plan.full * plan.blocks + index] = tile.reshape(
            plan.slots, SUBLANES, LANES
        ).astype(out_ref.dtype)


def other_kernel(
    plan, packed_ref, acc_ref, gate_ref, up_ref, down_ref, hidden_ref, out_ref, rows_ref
):
    unpack_rows(plan, packed_ref, rows_ref)
    first = pl.multiple_of((1 - lax.axis_index("rep")) * plan.feat, LANES)
    hid = gate_ref.shape[1]
    rows = rows_ref[...]
    gate = acc_ref[:, :hid] + jnp.dot(
        rows, gate_ref[pl.ds(first, plan.feat), :], preferred_element_type=F32
    )
    up = acc_ref[:, hid:] + jnp.dot(
        rows, up_ref[pl.ds(first, plan.feat), :], preferred_element_type=F32
    )
    hidden = (gate / (1.0 + jnp.exp(-gate)) * up).astype(BF16)
    if plan.full:
        hidden_ref[: plan.main_rows] = hidden[: plan.main_rows]
    if plan.tail:
        shape = (plan.tail_wide, plan.tail_rows)
        line, col = iota(shape, 0), iota(shape, 1)
        sender = floor_div(line, SUBLANES)
        spot = line - sender * SUBLANES
        spot = spot - floor_div(spot, plan.tail) * plan.tail
        hot = jnp.where(sender * plan.tail + spot == col, 1.0, 0.0).astype(BF16)
        hidden_ref[plan.main_rows :] = jnp.dot(
            hot, hidden[plan.main_rows :], preferred_element_type=F32
        ).astype(BF16)
    product = jnp.dot(
        hidden_ref[...], down_ref[:, pl.ds(first, plan.feat)], preferred_element_type=F32
    )
    emit_packed(plan, product, out_ref)


def down_kernel(plan, hidden_ref, down_ref, out_ref):
    first = pl.multiple_of(lax.axis_index("rep") * plan.feat, LANES)
    product = jnp.dot(
        hidden_ref[...], down_ref[:, pl.ds(first, plan.feat)], preferred_element_type=F32
    )
    emit_packed(plan, product, out_ref)


def sum_kernel(mine_ref, other_ref, out_ref):
    out_ref[...] = (mine_ref[...] + other_ref[...].astype(F32)).astype(BF16)


def combine_kernel(plan, pick_ref, column_ref, packed_ref, out_ref):
    for block in range(plan.blocks):
        stack = []
        if plan.full == 1:
            stack.append(packed_ref[:, block].astype(F32).reshape(plan.main_rows, LANES))
        elif plan.full:
            tiles = [
                packed_ref[:, index * plan.blocks + block].astype(F32)[:, None]
                for index in range(plan.full)
            ]
            stack.append(jnp.concatenate(tiles, axis=1).reshape(plan.main_rows, LANES))
        part = 0
        if plan.tail:
            index, part = divmod(block, plan.group)
            tile = packed_ref[:, plan.full * plan.blocks + index]
            stack.append(tile.astype(F32).reshape(plan.tail_wide, LANES))
        table = jnp.concatenate(stack, axis=0).astype(BF16)
        total = jnp.zeros((plan.tok, LANES), F32)
        for k in range(plan.choices):
            picked = jnp.dot(
                pick_ref[k * plan.parts + part], table, preferred_element_type=F32
            )
            total = total + column_ref[:, k : k + 1] * picked
        out_ref[:, lane_block(block)] = total.astype(BF16)


VMEM = pl.BlockSpec(memory_space=pltpu.VMEM)
ANY = pl.BlockSpec(memory_space=pltpu.HBM)


def call(kernel, in_specs, out_shape, flops, moved, limit, scratch=()):
    single = not isinstance(out_shape, (list, tuple))
    return pl.pallas_call(
        kernel,
        in_specs=in_specs,
        out_specs=VMEM if single else [VMEM] * len(out_shape),
        out_shape=out_shape,
        scratch_shapes=list(scratch),
        cost_estimate=pl.CostEstimate(flops=flops, bytes_accessed=moved, transcendentals=0),
        compiler_params=pltpu.CompilerParams(vmem_limit_bytes=limit),
    )


def body(tokens, expert_ids, gate_values, slot_expert, gate_weight, up_weight, down_weight):
    tok, choices = expert_ids.shape
    feat = tokens.shape[1]
    slots = slot_expert.shape[0]
    plan = Plan(tok, choices, feat, slots)
    weights = [gate_weight[0], up_weight[0], down_weight[0]]
    hid = weights[0].shape[1]
    gate_local, up_local, down_local = weights
    swap = [(0, 1), (1, 0)]
    packed_bytes = 2 * slots * plan.tiles * SUBLANES * LANES
    half_flops = 4 * plan.rows * feat * hid
    rows_scratch = pltpu.VMEM((plan.rows, feat), BF16)
    packed = jax.ShapeDtypeStruct(plan.packed, BF16)

    slot_row, ids, gates = slot_expert.reshape(1, slots), expert_ids.T, gate_values.T

    warm = call(
        warm_kernel,
        [],
        jax.ShapeDtypeStruct((SUBLANES, LANES), F32),
        COVER_FLOPS,
        COVER_BYTES,
        1 * MIB,
    )()
    send, found = call(
        functools.partial(pack_kernel, plan),
        [VMEM] * 4,
        [packed, jax.ShapeDtypeStruct((2 * choices, tok), jnp.int32)],
        COVER_FLOPS,
        COVER_BYTES,
        8 * MIB,
    )(warm, slot_row, ids, tokens)
    arrived = exchange(send, slots)
    partner = lax.ppermute(arrived, "rep", swap)
    acc = call(
        functools.partial(own_kernel, plan),
        [VMEM] * 4,
        jax.ShapeDtypeStruct((plan.rows, 2 * hid), F32),
        1 << 10,
        1 << 10,
        8 * MIB,
        [rows_scratch],
    )(arrived, gate_local, up_local, down_local)
    picks, columns = call(
        functools.partial(select_kernel, plan),
        [VMEM, VMEM],
        [
            jax.ShapeDtypeStruct((choices * plan.parts, tok, plan.wide), BF16),
            jax.ShapeDtypeStruct((tok, choices), F32),
        ],
        1 << 10,
        1 << 10,
        4 * MIB,
    )(found, gates)
    hidden, outbound = call(
        functools.partial(other_kernel, plan),
        [VMEM, VMEM, VMEM, VMEM, VMEM],
        [jax.ShapeDtypeStruct((plan.wide, hid), BF16), packed],
        half_flops + 2 * plan.wide * hid * feat,
        2 * packed_bytes + 8 * plan.rows * hid,
        8 * MIB,
        [rows_scratch],
    )(partner, acc, gate_local, up_local, down_local)
    received = lax.ppermute(outbound, "rep", swap)
    mine = call(
        functools.partial(down_kernel, plan),
        [VMEM, VMEM],
        jax.ShapeDtypeStruct(plan.packed, F32),
        2 * plan.wide * hid * feat,
        2 * packed_bytes,
        8 * MIB,
    )(hidden, down_local)
    result = call(
        sum_kernel, [VMEM, VMEM], packed, packed_bytes, 4 * packed_bytes, 4 * MIB
    )(mine, received)
    returned = exchange(result, slots)
    return call(
        functools.partial(combine_kernel, plan),
        [VMEM, VMEM, VMEM],
        jax.ShapeDtypeStruct((tok, feat), BF16),
        2 * tok * feat * plan.wide * choices,
        2 * packed_bytes,
        8 * MIB,
    )(picks, columns, returned)


def solution(mesh):
    assert mesh.shape["rep"] == 2
    return jax.shard_map(
        body,
        mesh=mesh,
        in_specs=(
            P(("groups", "ep"), "rep"),
            P(("groups", "ep"), None),
            P(("groups", "ep"), None),
            P(),
            P("ep", None, "rep"),
            P("ep", None, "rep"),
            P("ep", "rep", None),
        ),
        out_specs=P(("groups", "ep"), "rep"),
        check_vma=False,
    )
```

```python
import functools

import jax
import jax.numpy as jnp
from jax import lax
from jax.experimental import pallas as pl
from jax.experimental.pallas import tpu as pltpu
from jax.sharding import PartitionSpec as P


LANES = 128
SUBLANES = 8
MIB = 1 << 20
F32 = jnp.float32
BF16 = jnp.bfloat16
COVER_FLOPS = 1 << 34
COVER_BYTES = 1 << 25


class Plan:
    def __init__(self, tok, choices, feat, slots):
        experts = slots // 2
        self.tok, self.choices, self.feat, self.slots = tok, choices, feat, slots
        self.capacity = tok * choices * 5 // (4 * experts)
        assert feat % LANES == 0
        self.blocks = feat // LANES
        self.full = self.capacity // SUBLANES
        self.main = self.full * SUBLANES
        self.tail = self.capacity - self.main
        self.group = SUBLANES // self.tail if self.tail else 0
        self.tail_tiles = -(-self.blocks // self.group) if self.tail else 0
        self.tiles = self.full * self.blocks + self.tail_tiles
        self.main_rows = slots * self.main
        self.tail_rows = slots * self.tail
        self.rows = self.main_rows + self.tail_rows
        self.tail_wide = slots * SUBLANES if self.tail else 0
        self.wide = self.main_rows + self.tail_wide
        self.parts = max(1, self.group)
        self.packed = (slots, self.tiles, SUBLANES, LANES)


def iota(shape, dim):
    return lax.broadcasted_iota(jnp.int32, shape, dim)


def floor_div(values, divisor):
    return jnp.floor((values.astype(F32) + 0.5) * (1.0 / divisor)).astype(jnp.int32)


def exchange_place(index, members):
    away = index - 1 - members // 2
    away = jnp.where(index == 0, members // 2 - 1, away)
    return jnp.where(away >= 0, 2 * away, -2 * away - 1)


def exchange_order(members):
    away = [index // 2 if index % 2 == 0 else -(index // 2) - 1 for index in range(members)]
    return [(1 + members // 2 + step) % members for step in away]


def exchange(array, members):
    return lax.all_to_all(
        array,
        "ep",
        split_axis=0,
        concat_axis=0,
        tiled=True,
        axis_index_groups=[exchange_order(members)],
    )


def to_column(row):
    size = row.shape[1]
    diagonal = iota((size, size), 0) == iota((size, size), 1)
    return jnp.sum(jnp.where(diagonal, jnp.broadcast_to(row, (size, size)), 0), axis=1, keepdims=True)


def route(plan, member, slot_row, ids):
    slots, tok = plan.slots, plan.tok
    square = (slots, slots)
    row = slot_row.astype(F32)
    col = to_column(row)
    same = jnp.where(col == row, 1.0, 0.0)
    copies = jnp.sum(same, axis=1, keepdims=True)
    rank = jnp.sum(jnp.where(iota(square, 1) < iota(square, 0), same, 0.0), axis=1, keepdims=True)
    want = jnp.zeros((slots, 1), F32)
    for number in (2, 3, 4):
        want = jnp.where(copies == number, lax.rem(member, number).astype(F32), want)
    chosen = rank == want
    hits = [
        jnp.where((ids[k : k + 1].astype(F32) == col) & chosen, 1.0, 0.0)
        for k in range(plan.choices)
    ]
    before = jnp.where(iota((tok, tok), 0) < iota((tok, tok), 1), 1.0, 0.0).astype(BF16)
    counts = jnp.dot(sum(hits).astype(BF16), before, preferred_element_type=F32)
    line = exchange_place(iota((slots, tok), 0), slots).astype(F32)
    found = []
    for hit in hits:
        slot = jnp.sum(hit * line, axis=0, keepdims=True).astype(jnp.int32)
        place = jnp.sum(hit * counts, axis=0, keepdims=True).astype(jnp.int32)
        found.append((slot, place))
    return found


def main_code(plan, slot, place):
    return jnp.where(place < plan.main, slot * plan.main + place, -1)


def tail_code(plan, slot, place, part):
    spot = slot * SUBLANES + place - plan.main + part * plan.tail
    return jnp.where(place < plan.main, -1, spot)


def lane_block(index):
    return slice(index * LANES, (index + 1) * LANES)


def warm_kernel(out_ref):
    out_ref[...] = jnp.zeros_like(out_ref)


def read_found(plan, found_ref):
    lines = [found_ref[index : index + 1] for index in range(2 * plan.choices)]
    return list(zip(lines[: plan.choices], lines[plan.choices :], strict=True))


def pack_kernel(plan, warm_ref, slot_ref, ids_ref, tokens_ref, send_ref, found_ref):
    found = route(plan, lax.axis_index("ep"), slot_ref[...], ids_ref[...])
    for k, (slot, place) in enumerate(found):
        found_ref[k : k + 1] = slot
        found_ref[plan.choices + k : plan.choices + k + 1] = place
    if plan.full:
        line = iota((plan.main_rows, plan.tok), 0)
        hot = sum(jnp.where(line == main_code(plan, *pair), 1.0, 0.0) for pair in found)
        main = jnp.dot(hot.astype(BF16), tokens_ref[...], preferred_element_type=F32)
        for block in range(plan.blocks):
            tile = main[:, lane_block(block)].reshape(plan.slots, plan.full, SUBLANES, LANES)
            for index in range(plan.full):
                send_ref[:, index * plan.blocks + block] = tile[:, index].astype(BF16)
    if plan.tail:
        line = iota((plan.tail_wide, plan.tok * plan.group), 0)
        hot = jnp.zeros(line.shape, F32)
        for pair in found:
            codes = [tail_code(plan, *pair, part) for part in range(plan.group)]
            hot += jnp.where(line == jnp.concatenate(codes, axis=1), 1.0, 0.0)
        hot = hot.astype(BF16)
        for index in range(plan.tail_tiles):
            stack = []
            for part in range(plan.group):
                block = index * plan.group + part
                if block < plan.blocks:
                    stack.append(tokens_ref[:, lane_block(block)])
                else:
                    stack.append(jnp.zeros((plan.tok, LANES), BF16))
            tile = jnp.dot(hot, jnp.concatenate(stack, axis=0), preferred_element_type=F32)
            send_ref[:, plan.full * plan.blocks + index] = tile.reshape(
                plan.slots, SUBLANES, LANES
            ).astype(BF16)


def select_kernel(plan, found_ref, gates_ref, pick_ref, column_ref):
    lane = iota((plan.tok, plan.wide), 1).astype(F32)
    for k, (slot, place) in enumerate(read_found(plan, found_ref)):
        column_ref[:, k : k + 1] = to_column(gates_ref[k : k + 1])
        for part in range(plan.parts):
            tail = plan.main_rows + tail_code(plan, slot, place, part)
            code = jnp.where(place < plan.main, main_code(plan, slot, place), tail)
            pick = jnp.where(to_column(code.astype(F32)) == lane, 1.0, 0.0)
            pick_ref[k * plan.parts + part] = pick.astype(BF16)


def flat_tile(tile):
    return tile.astype(F32).reshape(-1, LANES).astype(BF16)


def unpack_rows(plan, packed_ref, rows_ref):
    for block in range(plan.blocks):
        for index in range(plan.full):
            tile = packed_ref[:, index * plan.blocks + block]
            if plan.full == 1:
                rows_ref[0 : plan.main_rows, lane_block(block)] = flat_tile(tile)
            else:
                for sender in range(plan.slots):
                    first = sender * plan.main + index * SUBLANES
                    rows_ref[first : first + SUBLANES, lane_block(block)] = tile[sender]
    if plan.tail:
        shape = (plan.group * plan.tail_rows, plan.tail_wide)
        line = iota(shape, 0)
        part = floor_div(line, plan.tail_rows)
        inner = line - part * plan.tail_rows
        sender = floor_div(inner, plan.tail)
        spot = sender * SUBLANES + part * plan.tail + inner - sender * plan.tail
        hot = jnp.where(spot == iota(shape, 1), 1.0, 0.0).astype(BF16)
        for index in range(plan.tail_tiles):
            tile = flat_tile(packed_ref[:, plan.full * plan.blocks + index])
            moved = jnp.dot(hot, tile, preferred_element_type=F32).astype(BF16)
            for part in range(plan.group):
                block = index * plan.group + part
                if block < plan.blocks:
                    rows_ref[plan.main_rows : plan.rows, lane_block(block)] = moved[
                        part * plan.tail_rows : (part + 1) * plan.tail_rows
                    ]


def own_kernel(plan, packed_ref, gate_ref, up_ref, down_ref, acc_ref, rows_ref):
    unpack_rows(plan, packed_ref, rows_ref)
    first = pl.multiple_of(lax.axis_index("rep") * plan.feat, LANES)
    hid = gate_ref.shape[1]
    rows = rows_ref[...]
    acc_ref[:, :hid] = jnp.dot(
        rows, gate_ref[pl.ds(first, plan.feat), :], preferred_element_type=F32
    )
    acc_ref[:, hid:] = jnp.dot(
        rows, up_ref[pl.ds(first, plan.feat), :], preferred_element_type=F32
    )


def emit_packed(plan, product, out_ref):
    for block in range(plan.blocks):
        tile = product[: plan.main_rows, lane_block(block)].reshape(
            plan.slots, plan.full, SUBLANES, LANES
        )
        for index in range(plan.full):
            out_ref[:, index * plan.blocks + block] = tile[:, index].astype(out_ref.dtype)
    for index in range(plan.tail_tiles):
        spot = iota((plan.tail_wide, LANES), 0)
        spot = spot - floor_div(spot, SUBLANES) * SUBLANES
        tile = jnp.zeros((plan.tail_wide, LANES), F32)
        for part in range(plan.group):
            block = index * plan.group + part
            if block < plan.blocks:
                here = (spot >= part * plan.tail) & (spot < (part + 1) * plan.tail)
                tile = jnp.where(here, product[plan.main_rows :, lane_block(block)], tile)
        out_ref[:, plan.full * plan.blocks + index] = tile.reshape(
            plan.slots, SUBLANES, LANES
        ).astype(out_ref.dtype)


def other_kernel(plan, packed_ref, acc_ref, gate_ref, up_ref, hidden_ref, rows_ref):
    unpack_rows(plan, packed_ref, rows_ref)
    first = pl.multiple_of((1 - lax.axis_index("rep")) * plan.feat, LANES)
    hid = gate_ref.shape[1]
    rows = rows_ref[...]
    gate = acc_ref[:, :hid] + jnp.dot(
        rows, gate_ref[pl.ds(first, plan.feat), :], preferred_element_type=F32
    )
    up = acc_ref[:, hid:] + jnp.dot(
        rows, up_ref[pl.ds(first, plan.feat), :], preferred_element_type=F32
    )
    hidden_ref[...] = (gate / (1.0 + jnp.exp(-gate)) * up).astype(BF16)


def down_product(plan, hidden_ref, down_ref):
    rows = [hidden_ref[: plan.main_rows]] if plan.full else []
    if plan.tail:
        shape = (plan.tail_wide, plan.tail_rows)
        line, col = iota(shape, 0), iota(shape, 1)
        sender = floor_div(line, SUBLANES)
        spot = line - sender * SUBLANES
        spot = spot - floor_div(spot, plan.tail) * plan.tail
        hot = jnp.where(sender * plan.tail + spot == col, 1.0, 0.0).astype(BF16)
        tail = jnp.dot(hot, hidden_ref[plan.main_rows :], preferred_element_type=F32)
        rows.append(tail.astype(BF16))
    first = pl.multiple_of(lax.axis_index("rep") * plan.feat, LANES)
    return jnp.dot(
        jnp.concatenate(rows, axis=0),
        down_ref[:, pl.ds(first, plan.feat)],
        preferred_element_type=F32,
    )


def down_own_kernel(plan, hidden_ref, down_ref, out_ref):
    out_ref[...] = down_product(plan, hidden_ref, down_ref)


def down_other_kernel(plan, hidden_ref, down_ref, mine_ref, out_ref):
    emit_packed(plan, mine_ref[...] + down_product(plan, hidden_ref, down_ref), out_ref)


def combine_kernel(plan, pick_ref, column_ref, packed_ref, out_ref):
    for block in range(plan.blocks):
        stack = []
        if plan.full == 1:
            stack.append(packed_ref[:, block].astype(F32).reshape(plan.main_rows, LANES))
        elif plan.full:
            tiles = [
                packed_ref[:, index * plan.blocks + block].astype(F32)[:, None]
                for index in range(plan.full)
            ]
            stack.append(jnp.concatenate(tiles, axis=1).reshape(plan.main_rows, LANES))
        part = 0
        if plan.tail:
            index, part = divmod(block, plan.group)
            tile = packed_ref[:, plan.full * plan.blocks + index]
            stack.append(tile.astype(F32).reshape(plan.tail_wide, LANES))
        table = jnp.concatenate(stack, axis=0).astype(BF16)
        total = jnp.zeros((plan.tok, LANES), F32)
        for k in range(plan.choices):
            picked = jnp.dot(
                pick_ref[k * plan.parts + part], table, preferred_element_type=F32
            )
            total = total + column_ref[:, k : k + 1] * picked
        out_ref[:, lane_block(block)] = total.astype(BF16)


VMEM = pl.BlockSpec(memory_space=pltpu.VMEM)
ANY = pl.BlockSpec(memory_space=pltpu.HBM)


def call(kernel, in_specs, out_shape, flops, moved, limit, scratch=()):
    single = not isinstance(out_shape, (list, tuple))
    return pl.pallas_call(
        kernel,
        in_specs=in_specs,
        out_specs=VMEM if single else [VMEM] * len(out_shape),
        out_shape=out_shape,
        scratch_shapes=list(scratch),
        cost_estimate=pl.CostEstimate(flops=flops, bytes_accessed=moved, transcendentals=0),
        compiler_params=pltpu.CompilerParams(vmem_limit_bytes=limit),
    )


def body(tokens, expert_ids, gate_values, slot_expert, gate_weight, up_weight, down_weight):
    tok, choices = expert_ids.shape
    feat = tokens.shape[1]
    slots = slot_expert.shape[0]
    plan = Plan(tok, choices, feat, slots)
    weights = [gate_weight[0], up_weight[0], down_weight[0]]
    hid = weights[0].shape[1]
    gate_local, up_local, down_local = weights
    swap = [(0, 1), (1, 0)]
    packed_bytes = 2 * slots * plan.tiles * SUBLANES * LANES
    half_flops = 4 * plan.rows * feat * hid
    rows_scratch = pltpu.VMEM((plan.rows, feat), BF16)
    packed = jax.ShapeDtypeStruct(plan.packed, BF16)

    slot_row, ids, gates = slot_expert.reshape(1, slots), expert_ids.T, gate_values.T

    down_swapped = lax.ppermute(down_local, "rep", swap)
    warm = call(
        warm_kernel,
        [],
        jax.ShapeDtypeStruct((SUBLANES, LANES), F32),
        COVER_FLOPS,
        COVER_BYTES,
        1 * MIB,
    )()
    send, found = call(
        functools.partial(pack_kernel, plan),
        [VMEM] * 4,
        [packed, jax.ShapeDtypeStruct((2 * choices, tok), jnp.int32)],
        COVER_FLOPS,
        COVER_BYTES,
        8 * MIB,
    )(warm, slot_row, ids, tokens)
    arrived = exchange(send, slots)
    partner = lax.ppermute(arrived, "rep", swap)
    acc = call(
        functools.partial(own_kernel, plan),
        [VMEM] * 4,
        jax.ShapeDtypeStruct((plan.rows, 2 * hid), F32),
        1 << 10,
        1 << 10,
        8 * MIB,
        [rows_scratch],
    )(arrived, gate_local, up_local, down_local)
    picks, columns = call(
        functools.partial(select_kernel, plan),
        [VMEM, VMEM],
        [
            jax.ShapeDtypeStruct((choices * plan.parts, tok, plan.wide), BF16),
            jax.ShapeDtypeStruct((tok, choices), F32),
        ],
        1 << 10,
        1 << 10,
        4 * MIB,
    )(found, gates)
    hidden = call(
        functools.partial(other_kernel, plan),
        [VMEM] * 4,
        jax.ShapeDtypeStruct((plan.rows, hid), BF16),
        half_flops,
        packed_bytes + 8 * plan.rows * hid,
        8 * MIB,
        [rows_scratch],
    )(partner, acc, gate_local, up_local)
    received = lax.ppermute(hidden, "rep", swap)
    mine = call(
        functools.partial(down_own_kernel, plan),
        [VMEM] * 2,
        jax.ShapeDtypeStruct((plan.wide, feat), F32),
        2 * plan.wide * hid * feat,
        2 * packed_bytes,
        8 * MIB,
    )(hidden, down_local)
    result = call(
        functools.partial(down_other_kernel, plan),
        [VMEM] * 3,
        packed,
        2 * plan.wide * hid * feat,
        2 * packed_bytes,
        8 * MIB,
    )(received, down_swapped, mine)
    returned = exchange(result, slots)
    return call(
        functools.partial(combine_kernel, plan),
        [VMEM, VMEM, VMEM],
        jax.ShapeDtypeStruct((tok, feat), BF16),
        2 * tok * feat * plan.wide * choices,
        2 * packed_bytes,
        8 * MIB,
    )(picks, columns, returned)


def solution(mesh):
    assert mesh.shape["rep"] == 2
    return jax.shard_map(
        body,
        mesh=mesh,
        in_specs=(
            P(("groups", "ep"), "rep"),
            P(("groups", "ep"), None),
            P(("groups", "ep"), None),
            P(),
            P("ep", None, "rep"),
            P("ep", None, "rep"),
            P("ep", "rep", None),
        ),
        out_specs=P(("groups", "ep"), "rep"),
        check_vma=False,
    )
```

```python
import functools

import jax
import jax.numpy as jnp
from jax import lax
from jax.experimental import pallas as pl
from jax.experimental.pallas import tpu as pltpu
from jax.sharding import PartitionSpec as P


LANES = 128
TILE_ROWS = 4
MIB = 1 << 20
F32 = jnp.float32
BF16 = jnp.bfloat16
COVER_FLOPS = 1 << 34
COVER_BYTES = 1 << 25


class Plan:
    def __init__(self, tok, choices, feat, slots):
        experts = slots // 2
        self.tok, self.choices, self.feat, self.slots = tok, choices, feat, slots
        self.capacity = tok * choices * 5 // (4 * experts)
        assert feat % LANES == 0
        self.blocks = feat // LANES
        self.full = self.capacity // TILE_ROWS
        self.main = self.full * TILE_ROWS
        self.tail = self.capacity - self.main
        self.group = TILE_ROWS // self.tail if self.tail else 0
        self.tail_tiles = -(-self.blocks // self.group) if self.tail else 0
        self.tiles = self.full * self.blocks + self.tail_tiles
        self.main_rows = slots * self.main
        self.tail_rows = slots * self.tail
        self.rows = self.main_rows + self.tail_rows
        self.tail_wide = slots * TILE_ROWS if self.tail else 0
        self.wide = self.main_rows + self.tail_wide
        self.parts = max(1, self.group)
        self.packed = (slots, self.tiles, TILE_ROWS, LANES)


def iota(shape, dim):
    return lax.broadcasted_iota(jnp.int32, shape, dim)


def floor_div(values, divisor):
    return jnp.floor((values.astype(F32) + 0.5) * (1.0 / divisor)).astype(jnp.int32)


def exchange_place(index, members):
    away = index - 1 - members // 2
    away = jnp.where(index == 0, members // 2 - 1, away)
    return jnp.where(away >= 0, 2 * away, -2 * away - 1)


def exchange_order(members):
    away = [index // 2 if index % 2 == 0 else -(index // 2) - 1 for index in range(members)]
    return [(1 + members // 2 + step) % members for step in away]


def exchange(array, members):
    return lax.all_to_all(
        array,
        "ep",
        split_axis=0,
        concat_axis=0,
        tiled=True,
        axis_index_groups=[exchange_order(members)],
    )


def to_column(row):
    size = row.shape[1]
    diagonal = iota((size, size), 0) == iota((size, size), 1)
    return jnp.sum(jnp.where(diagonal, jnp.broadcast_to(row, (size, size)), 0), axis=1, keepdims=True)


def route(plan, member, slot_row, ids):
    slots, tok = plan.slots, plan.tok
    square = (slots, slots)
    col = to_column(slot_row.astype(F32))
    same = jnp.where(col == slot_row.astype(F32), 1.0, 0.0)
    copies = jnp.sum(same, axis=1, keepdims=True)
    rank = jnp.sum(jnp.where(iota(square, 1) < iota(square, 0), same, 0.0), axis=1, keepdims=True)
    want = jnp.zeros((slots, 1), F32)
    for number in (2, 3, 4):
        want = jnp.where(copies == number, lax.rem(member, number).astype(F32), want)
    chosen = rank == want
    line = exchange_place(iota((slots, tok), 0), slots).astype(F32)
    rows = [ids[k : k + 1].astype(F32) for k in range(plan.choices)]
    cols = [to_column(row) for row in rows]
    before = iota((tok, tok), 0) < iota((tok, tok), 1)
    found = []
    for row in rows:
        slot = jnp.sum(jnp.where((row == col) & chosen, line, 0.0), axis=0, keepdims=True)
        earlier = sum(jnp.where((other == row) & before, 1.0, 0.0) for other in cols)
        place = jnp.sum(earlier, axis=0, keepdims=True)
        found.append((slot.astype(jnp.int32), place.astype(jnp.int32)))
    return found


def main_code(plan, slot, place):
    return jnp.where(place < plan.main, slot * plan.main + place, -1)


def tail_code(plan, slot, place, part):
    spot = slot * TILE_ROWS + place - plan.main + part * plan.tail
    return jnp.where(place < plan.main, -1, spot)


def lane_block(index):
    return slice(index * LANES, (index + 1) * LANES)


def warm_kernel(out_ref):
    out_ref[...] = jnp.zeros_like(out_ref)


def read_found(plan, found_ref):
    lines = [found_ref[index : index + 1] for index in range(2 * plan.choices)]
    return list(zip(lines[: plan.choices], lines[plan.choices :], strict=True))


def pack_kernel(plan, warm_ref, slot_ref, ids_ref, tokens_ref, send_ref, found_ref):
    found = route(plan, lax.axis_index("ep"), slot_ref[...], ids_ref[...])
    for k, (slot, place) in enumerate(found):
        found_ref[k : k + 1] = slot
        found_ref[plan.choices + k : plan.choices + k + 1] = place
    if plan.full:
        line = iota((plan.main_rows, plan.tok), 0)
        hot = sum(jnp.where(line == main_code(plan, *pair), 1.0, 0.0) for pair in found)
        main = jnp.dot(hot.astype(BF16), tokens_ref[...], preferred_element_type=F32)
        for block in range(plan.blocks):
            tile = main[:, lane_block(block)].reshape(plan.slots, plan.full, TILE_ROWS, LANES)
            for index in range(plan.full):
                send_ref[:, index * plan.blocks + block] = tile[:, index].astype(BF16)
    if plan.tail:
        line = iota((plan.tail_wide, plan.tok * plan.group), 0)
        hot = jnp.zeros(line.shape, F32)
        for pair in found:
            codes = [tail_code(plan, *pair, part) for part in range(plan.group)]
            hot += jnp.where(line == jnp.concatenate(codes, axis=1), 1.0, 0.0)
        hot = hot.astype(BF16)
        for index in range(plan.tail_tiles):
            stack = []
            for part in range(plan.group):
                block = index * plan.group + part
                if block < plan.blocks:
                    stack.append(tokens_ref[:, lane_block(block)])
                else:
                    stack.append(jnp.zeros((plan.tok, LANES), BF16))
            tile = jnp.dot(hot, jnp.concatenate(stack, axis=0), preferred_element_type=F32)
            send_ref[:, plan.full * plan.blocks + index] = tile.reshape(
                plan.slots, TILE_ROWS, LANES
            ).astype(BF16)


def select_kernel(plan, found_ref, gates_ref, pick_ref, column_ref):
    lane = iota((plan.tok, plan.wide), 1).astype(F32)
    for k, (slot, place) in enumerate(read_found(plan, found_ref)):
        column_ref[:, k : k + 1] = to_column(gates_ref[k : k + 1])
        for part in range(plan.parts):
            tail = plan.main_rows + tail_code(plan, slot, place, part)
            code = jnp.where(place < plan.main, main_code(plan, slot, place), tail)
            pick = jnp.where(to_column(code.astype(F32)) == lane, 1.0, 0.0)
            pick_ref[k * plan.parts + part] = pick.astype(BF16)


def flat_tile(tile):
    return tile.astype(F32).reshape(-1, LANES).astype(BF16)


def unpack_rows(plan, packed_ref, rows_ref):
    for block in range(plan.blocks):
        for index in range(plan.full):
            tile = packed_ref[:, index * plan.blocks + block]
            if plan.full == 1:
                rows_ref[0 : plan.main_rows, lane_block(block)] = flat_tile(tile)
            else:
                for sender in range(plan.slots):
                    first = sender * plan.main + index * TILE_ROWS
                    rows_ref[first : first + TILE_ROWS, lane_block(block)] = tile[sender]
    if plan.tail:
        shape = (plan.group * plan.tail_rows, plan.tail_wide)
        line = iota(shape, 0)
        part = floor_div(line, plan.tail_rows)
        inner = line - part * plan.tail_rows
        sender = floor_div(inner, plan.tail)
        spot = sender * TILE_ROWS + part * plan.tail + inner - sender * plan.tail
        hot = jnp.where(spot == iota(shape, 1), 1.0, 0.0).astype(BF16)
        for index in range(plan.tail_tiles):
            tile = flat_tile(packed_ref[:, plan.full * plan.blocks + index])
            moved = jnp.dot(hot, tile, preferred_element_type=F32).astype(BF16)
            for part in range(plan.group):
                block = index * plan.group + part
                if block < plan.blocks:
                    rows_ref[plan.main_rows : plan.rows, lane_block(block)] = moved[
                        part * plan.tail_rows : (part + 1) * plan.tail_rows
                    ]


def own_kernel(plan, packed_ref, gate_ref, up_ref, down_ref, acc_ref, rows_ref):
    unpack_rows(plan, packed_ref, rows_ref)
    first = pl.multiple_of(lax.axis_index("rep") * plan.feat, LANES)
    hid = gate_ref.shape[1]
    rows = rows_ref[...]
    acc_ref[:, :hid] = jnp.dot(
        rows, gate_ref[pl.ds(first, plan.feat), :], preferred_element_type=F32
    )
    acc_ref[:, hid:] = jnp.dot(
        rows, up_ref[pl.ds(first, plan.feat), :], preferred_element_type=F32
    )


def emit_packed(plan, product, out_ref):
    for block in range(plan.blocks):
        tile = product[: plan.main_rows, lane_block(block)].reshape(
            plan.slots, plan.full, TILE_ROWS, LANES
        )
        for index in range(plan.full):
            out_ref[:, index * plan.blocks + block] = tile[:, index].astype(out_ref.dtype)
    for index in range(plan.tail_tiles):
        spot = iota((plan.tail_wide, LANES), 0)
        spot = spot - floor_div(spot, TILE_ROWS) * TILE_ROWS
        tile = jnp.zeros((plan.tail_wide, LANES), F32)
        for part in range(plan.group):
            block = index * plan.group + part
            if block < plan.blocks:
                here = (spot >= part * plan.tail) & (spot < (part + 1) * plan.tail)
                tile = jnp.where(here, product[plan.main_rows :, lane_block(block)], tile)
        out_ref[:, plan.full * plan.blocks + index] = tile.reshape(
            plan.slots, TILE_ROWS, LANES
        ).astype(out_ref.dtype)


def other_kernel(plan, packed_ref, acc_ref, gate_ref, up_ref, hidden_ref, rows_ref):
    unpack_rows(plan, packed_ref, rows_ref)
    first = pl.multiple_of((1 - lax.axis_index("rep")) * plan.feat, LANES)
    hid = gate_ref.shape[1]
    rows = rows_ref[...]
    gate = acc_ref[:, :hid] + jnp.dot(
        rows, gate_ref[pl.ds(first, plan.feat), :], preferred_element_type=F32
    )
    up = acc_ref[:, hid:] + jnp.dot(
        rows, up_ref[pl.ds(first, plan.feat), :], preferred_element_type=F32
    )
    hidden_ref[...] = (gate / (1.0 + jnp.exp(-gate)) * up).astype(BF16)


def down_product(plan, hidden_ref, down_ref):
    rows = [hidden_ref[: plan.main_rows]] if plan.full else []
    if plan.tail:
        shape = (plan.tail_wide, plan.tail_rows)
        line, col = iota(shape, 0), iota(shape, 1)
        sender = floor_div(line, TILE_ROWS)
        spot = line - sender * TILE_ROWS
        spot = spot - floor_div(spot, plan.tail) * plan.tail
        hot = jnp.where(sender * plan.tail + spot == col, 1.0, 0.0).astype(BF16)
        tail = jnp.dot(hot, hidden_ref[plan.main_rows :], preferred_element_type=F32)
        rows.append(tail.astype(BF16))
    first = pl.multiple_of(lax.axis_index("rep") * plan.feat, LANES)
    return jnp.dot(
        jnp.concatenate(rows, axis=0),
        down_ref[:, pl.ds(first, plan.feat)],
        preferred_element_type=F32,
    )


def down_own_kernel(plan, hidden_ref, down_ref, out_ref):
    out_ref[...] = down_product(plan, hidden_ref, down_ref)


def down_other_kernel(plan, hidden_ref, down_ref, mine_ref, out_ref):
    emit_packed(plan, mine_ref[...] + down_product(plan, hidden_ref, down_ref), out_ref)


def combine_kernel(plan, pick_ref, column_ref, packed_ref, out_ref):
    for block in range(plan.blocks):
        stack = []
        if plan.full == 1:
            stack.append(packed_ref[:, block].astype(F32).reshape(plan.main_rows, LANES))
        elif plan.full:
            tiles = [
                packed_ref[:, index * plan.blocks + block].astype(F32)[:, None]
                for index in range(plan.full)
            ]
            stack.append(jnp.concatenate(tiles, axis=1).reshape(plan.main_rows, LANES))
        part = 0
        if plan.tail:
            index, part = divmod(block, plan.group)
            tile = packed_ref[:, plan.full * plan.blocks + index]
            stack.append(tile.astype(F32).reshape(plan.tail_wide, LANES))
        table = jnp.concatenate(stack, axis=0).astype(BF16)
        total = jnp.zeros((plan.tok, LANES), F32)
        for k in range(plan.choices):
            picked = jnp.dot(
                pick_ref[k * plan.parts + part], table, preferred_element_type=F32
            )
            total = total + column_ref[:, k : k + 1] * picked
        out_ref[:, lane_block(block)] = total.astype(BF16)


VMEM = pl.BlockSpec(memory_space=pltpu.VMEM)
ANY = pl.BlockSpec(memory_space=pltpu.HBM)


def call(kernel, in_specs, out_shape, flops, moved, limit, scratch=()):
    single = not isinstance(out_shape, (list, tuple))
    return pl.pallas_call(
        kernel,
        in_specs=in_specs,
        out_specs=VMEM if single else [VMEM] * len(out_shape),
        out_shape=out_shape,
        scratch_shapes=list(scratch),
        cost_estimate=pl.CostEstimate(flops=flops, bytes_accessed=moved, transcendentals=0),
        compiler_params=pltpu.CompilerParams(vmem_limit_bytes=limit),
    )


def body(tokens, expert_ids, gate_values, slot_expert, gate_weight, up_weight, down_weight):
    tok, choices = expert_ids.shape
    feat = tokens.shape[1]
    slots = slot_expert.shape[0]
    plan = Plan(tok, choices, feat, slots)
    weights = [gate_weight[0], up_weight[0], down_weight[0]]
    hid = weights[0].shape[1]
    gate_local, up_local, down_local = weights
    swap = [(0, 1), (1, 0)]
    packed_bytes = 2 * slots * plan.tiles * TILE_ROWS * LANES
    half_flops = 4 * plan.rows * feat * hid
    rows_scratch = pltpu.VMEM((plan.rows, feat), BF16)
    packed = jax.ShapeDtypeStruct(plan.packed, BF16)

    slot_row, ids, gates = slot_expert.reshape(1, slots), expert_ids.T, gate_values.T

    down_swapped = lax.ppermute(down_local, "rep", swap)
    warm = call(
        warm_kernel,
        [],
        jax.ShapeDtypeStruct((TILE_ROWS, LANES), F32),
        COVER_FLOPS,
        COVER_BYTES,
        1 * MIB,
    )()
    send, found = call(
        functools.partial(pack_kernel, plan),
        [VMEM] * 4,
        [packed, jax.ShapeDtypeStruct((2 * choices, tok), jnp.int32)],
        COVER_FLOPS,
        COVER_BYTES,
        8 * MIB,
    )(warm, slot_row, ids, tokens)
    arrived = exchange(send, slots)
    partner = lax.ppermute(arrived, "rep", swap)
    acc = call(
        functools.partial(own_kernel, plan),
        [VMEM] * 4,
        jax.ShapeDtypeStruct((plan.rows, 2 * hid), F32),
        1 << 10,
        1 << 10,
        8 * MIB,
        [rows_scratch],
    )(arrived, gate_local, up_local, down_local)
    picks, columns = call(
        functools.partial(select_kernel, plan),
        [VMEM, VMEM],
        [
            jax.ShapeDtypeStruct((choices * plan.parts, tok, plan.wide), BF16),
            jax.ShapeDtypeStruct((tok, choices), F32),
        ],
        1 << 10,
        1 << 10,
        4 * MIB,
    )(found, gates)
    hidden = call(
        functools.partial(other_kernel, plan),
        [VMEM] * 4,
        jax.ShapeDtypeStruct((plan.rows, hid), BF16),
        half_flops,
        packed_bytes + 8 * plan.rows * hid,
        8 * MIB,
        [rows_scratch],
    )(partner, acc, gate_local, up_local)
    received = lax.ppermute(hidden, "rep", swap)
    mine = call(
        functools.partial(down_own_kernel, plan),
        [VMEM] * 2,
        jax.ShapeDtypeStruct((plan.wide, feat), F32),
        2 * plan.wide * hid * feat,
        2 * packed_bytes,
        8 * MIB,
    )(hidden, down_local)
    result = call(
        functools.partial(down_other_kernel, plan),
        [VMEM] * 3,
        packed,
        2 * plan.wide * hid * feat,
        2 * packed_bytes,
        8 * MIB,
    )(received, down_swapped, mine)
    returned = exchange(result, slots)
    return call(
        functools.partial(combine_kernel, plan),
        [VMEM, VMEM, VMEM],
        jax.ShapeDtypeStruct((tok, feat), BF16),
        2 * tok * feat * plan.wide * choices,
        2 * packed_bytes,
        8 * MIB,
    )(picks, columns, returned)


def solution(mesh):
    assert mesh.shape["rep"] == 2
    return jax.shard_map(
        body,
        mesh=mesh,
        in_specs=(
            P(("groups", "ep"), "rep"),
            P(("groups", "ep"), None),
            P(("groups", "ep"), None),
            P(),
            P("ep", None, "rep"),
            P("ep", None, "rep"),
            P("ep", "rep", None),
        ),
        out_specs=P(("groups", "ep"), "rep"),
        check_vma=False,
    )
```

```python
import functools

import jax
import jax.numpy as jnp
from jax import lax
from jax.experimental import pallas as pl
from jax.experimental.pallas import tpu as pltpu
from jax.sharding import PartitionSpec as P


LANES = 128
TILE_ROWS = 4
MIB = 1 << 20
F32 = jnp.float32
BF16 = jnp.bfloat16
COVER_FLOPS = 1 << 34
COVER_BYTES = 1 << 25


class Plan:
    def __init__(self, tok, choices, feat, slots):
        experts = slots // 2
        self.tok, self.choices, self.feat, self.slots = tok, choices, feat, slots
        self.capacity = tok * choices * 5 // (4 * experts)
        assert feat % LANES == 0
        self.blocks = feat // LANES
        self.full = self.capacity // TILE_ROWS
        self.main = self.full * TILE_ROWS
        self.tail = self.capacity - self.main
        self.group = TILE_ROWS // self.tail if self.tail else 0
        self.tail_tiles = -(-self.blocks // self.group) if self.tail else 0
        self.tiles = self.full * self.blocks + self.tail_tiles
        self.main_rows = slots * self.main
        self.tail_rows = slots * self.tail
        self.rows = self.main_rows + self.tail_rows
        self.tail_wide = slots * TILE_ROWS if self.tail else 0
        self.wide = self.main_rows + self.tail_wide
        self.parts = max(1, self.group)
        self.packed = (slots, self.tiles, TILE_ROWS, LANES)


def iota(shape, dim):
    return lax.broadcasted_iota(jnp.int32, shape, dim)


def floor_div(values, divisor):
    return jnp.floor((values.astype(F32) + 0.5) * (1.0 / divisor)).astype(jnp.int32)


def exchange_place(index, members):
    away = index - 1 - members // 2
    away = jnp.where(index == 0, members // 2 - 1, away)
    return jnp.where(away >= 0, 2 * away, -2 * away - 1)


def exchange_order(members):
    away = [index // 2 if index % 2 == 0 else -(index // 2) - 1 for index in range(members)]
    return [(1 + members // 2 + step) % members for step in away]


def exchange(array, members):
    return lax.all_to_all(
        array,
        "ep",
        split_axis=0,
        concat_axis=0,
        tiled=True,
        axis_index_groups=[exchange_order(members)],
    )


def to_column(row):
    size = row.shape[1]
    diagonal = iota((size, size), 0) == iota((size, size), 1)
    return jnp.sum(jnp.where(diagonal, jnp.broadcast_to(row, (size, size)), 0), axis=1, keepdims=True)


def route(plan, member, slot_row, ids):
    slots, tok = plan.slots, plan.tok
    square = (slots, slots)
    col = to_column(slot_row.astype(F32))
    same = jnp.where(col == slot_row.astype(F32), 1.0, 0.0)
    copies = jnp.sum(same, axis=1, keepdims=True)
    rank = jnp.sum(jnp.where(iota(square, 1) < iota(square, 0), same, 0.0), axis=1, keepdims=True)
    want = jnp.zeros((slots, 1), F32)
    for number in (2, 3, 4):
        want = jnp.where(copies == number, lax.rem(member, number).astype(F32), want)
    chosen = rank == want
    line = exchange_place(iota((slots, tok), 0), slots).astype(F32)
    rows = [ids[k : k + 1].astype(F32) for k in range(plan.choices)]
    cols = [to_column(row) for row in rows]
    before = iota((tok, tok), 0) < iota((tok, tok), 1)
    found = []
    for row in rows:
        slot = jnp.sum(jnp.where((row == col) & chosen, line, 0.0), axis=0, keepdims=True)
        earlier = sum(jnp.where((other == row) & before, 1.0, 0.0) for other in cols)
        place = jnp.sum(earlier, axis=0, keepdims=True)
        found.append((slot.astype(jnp.int32), place.astype(jnp.int32)))
    return found


def main_code(plan, slot, place):
    return jnp.where(place < plan.main, slot * plan.main + place, -1)


def table_code(plan, slot, place, part):
    tile = sum((place >= (index + 1) * TILE_ROWS).astype(jnp.int32) for index in range(plan.full))
    inner = place - tile * TILE_ROWS + jnp.where(tile == plan.full, part * plan.tail, 0)
    return (tile * plan.slots + slot) * TILE_ROWS + inner


def tail_code(plan, slot, place, part):
    spot = slot * TILE_ROWS + place - plan.main + part * plan.tail
    return jnp.where(place < plan.main, -1, spot)


def lane_block(index):
    return slice(index * LANES, (index + 1) * LANES)


def warm_kernel(out_ref):
    out_ref[...] = jnp.zeros_like(out_ref)


def read_found(plan, found_ref):
    lines = [found_ref[index : index + 1] for index in range(2 * plan.choices)]
    return list(zip(lines[: plan.choices], lines[plan.choices :], strict=True))


def route_kernel(plan, warm_ref, slot_ref, ids_ref, found_ref):
    found = route(plan, lax.axis_index("ep"), slot_ref[...], ids_ref[...])
    for k, (slot, place) in enumerate(found):
        found_ref[k : k + 1] = slot
        found_ref[plan.choices + k : plan.choices + k + 1] = place


def pack_kernel(plan, found_ref, tokens_ref, send_ref):
    found = read_found(plan, found_ref)
    if plan.full:
        line = iota((plan.main_rows, plan.tok), 0)
        hot = sum(jnp.where(line == main_code(plan, *pair), 1.0, 0.0) for pair in found)
        main = jnp.dot(hot.astype(BF16), tokens_ref[...], preferred_element_type=F32)
        for block in range(plan.blocks):
            tile = main[:, lane_block(block)].reshape(plan.slots, plan.full, TILE_ROWS, LANES)
            for index in range(plan.full):
                send_ref[:, index * plan.blocks + block] = tile[:, index].astype(BF16)
    if plan.tail:
        line = iota((plan.tail_wide, plan.tok * plan.group), 0)
        hot = jnp.zeros(line.shape, F32)
        for pair in found:
            codes = [tail_code(plan, *pair, part) for part in range(plan.group)]
            hot += jnp.where(line == jnp.concatenate(codes, axis=1), 1.0, 0.0)
        hot = hot.astype(BF16)
        for index in range(plan.tail_tiles):
            stack = []
            for part in range(plan.group):
                block = index * plan.group + part
                if block < plan.blocks:
                    stack.append(tokens_ref[:, lane_block(block)])
                else:
                    stack.append(jnp.zeros((plan.tok, LANES), BF16))
            tile = jnp.dot(hot, jnp.concatenate(stack, axis=0), preferred_element_type=F32)
            send_ref[:, plan.full * plan.blocks + index] = tile.reshape(
                plan.slots, TILE_ROWS, LANES
            ).astype(BF16)


def select_kernel(plan, found_ref, gates_ref, pick_ref, column_ref):
    lane = iota((plan.tok, plan.wide), 1).astype(F32)
    for k, (slot, place) in enumerate(read_found(plan, found_ref)):
        column_ref[:, k : k + 1] = to_column(gates_ref[k : k + 1])
        for part in range(plan.parts):
            code = table_code(plan, slot, place, part)
            pick = jnp.where(to_column(code.astype(F32)) == lane, 1.0, 0.0)
            pick_ref[k * plan.parts + part] = pick.astype(BF16)


def flat_tile(tile):
    return tile.reshape(-1, LANES)


def unpack_rows(plan, packed_ref, rows_ref):
    for block in range(plan.blocks):
        for index in range(plan.full):
            tile = packed_ref[:, index * plan.blocks + block]
            if plan.full == 1:
                rows_ref[0 : plan.main_rows, lane_block(block)] = flat_tile(tile)
            else:
                for sender in range(plan.slots):
                    first = sender * plan.main + index * TILE_ROWS
                    rows_ref[first : first + TILE_ROWS, lane_block(block)] = tile[sender]
    if plan.tail:
        shape = (plan.group * plan.tail_rows, plan.tail_wide)
        line = iota(shape, 0)
        part = floor_div(line, plan.tail_rows)
        inner = line - part * plan.tail_rows
        sender = floor_div(inner, plan.tail)
        spot = sender * TILE_ROWS + part * plan.tail + inner - sender * plan.tail
        hot = jnp.where(spot == iota(shape, 1), 1.0, 0.0).astype(BF16)
        for index in range(plan.tail_tiles):
            tile = flat_tile(packed_ref[:, plan.full * plan.blocks + index])
            moved = jnp.dot(hot, tile, preferred_element_type=F32).astype(BF16)
            for part in range(plan.group):
                block = index * plan.group + part
                if block < plan.blocks:
                    rows_ref[plan.main_rows : plan.rows, lane_block(block)] = moved[
                        part * plan.tail_rows : (part + 1) * plan.tail_rows
                    ]


def own_kernel(plan, packed_ref, gate_ref, up_ref, down_ref, acc_ref, rows_ref):
    unpack_rows(plan, packed_ref, rows_ref)
    first = pl.multiple_of(lax.axis_index("rep") * plan.feat, LANES)
    hid = gate_ref.shape[1]
    rows = rows_ref[...]
    acc_ref[:, :hid] = jnp.dot(
        rows, gate_ref[pl.ds(first, plan.feat), :], preferred_element_type=F32
    )
    acc_ref[:, hid:] = jnp.dot(
        rows, up_ref[pl.ds(first, plan.feat), :], preferred_element_type=F32
    )


def emit_packed(plan, product, out_ref):
    for block in range(plan.blocks):
        tile = product[: plan.main_rows, lane_block(block)].reshape(
            plan.slots, plan.full, TILE_ROWS, LANES
        )
        for index in range(plan.full):
            out_ref[:, index * plan.blocks + block] = tile[:, index].astype(out_ref.dtype)
    for index in range(plan.tail_tiles):
        spot = iota((plan.tail_wide, LANES), 0)
        spot = spot - floor_div(spot, TILE_ROWS) * TILE_ROWS
        tile = jnp.zeros((plan.tail_wide, LANES), F32)
        for part in range(plan.group):
            block = index * plan.group + part
            if block < plan.blocks:
                here = (spot >= part * plan.tail) & (spot < (part + 1) * plan.tail)
                tile = jnp.where(here, product[plan.main_rows :, lane_block(block)], tile)
        out_ref[:, plan.full * plan.blocks + index] = tile.reshape(
            plan.slots, TILE_ROWS, LANES
        ).astype(out_ref.dtype)


def other_kernel(plan, packed_ref, acc_ref, gate_ref, up_ref, hidden_ref, rows_ref):
    unpack_rows(plan, packed_ref, rows_ref)
    first = pl.multiple_of((1 - lax.axis_index("rep")) * plan.feat, LANES)
    hid = gate_ref.shape[1]
    rows = rows_ref[...]
    gate = acc_ref[:, :hid] + jnp.dot(
        rows, gate_ref[pl.ds(first, plan.feat), :], preferred_element_type=F32
    )
    up = acc_ref[:, hid:] + jnp.dot(
        rows, up_ref[pl.ds(first, plan.feat), :], preferred_element_type=F32
    )
    hidden_ref[...] = (gate / (1.0 + jnp.exp(-gate)) * up).astype(BF16)


def down_product(plan, hidden_ref, down_ref):
    rows = [hidden_ref[: plan.main_rows]] if plan.full else []
    if plan.tail:
        shape = (plan.tail_wide, plan.tail_rows)
        line, col = iota(shape, 0), iota(shape, 1)
        sender = floor_div(line, TILE_ROWS)
        spot = line - sender * TILE_ROWS
        spot = spot - floor_div(spot, plan.tail) * plan.tail
        hot = jnp.where(sender * plan.tail + spot == col, 1.0, 0.0).astype(BF16)
        tail = jnp.dot(hot, hidden_ref[plan.main_rows :], preferred_element_type=F32)
        rows.append(tail.astype(BF16))
    first = pl.multiple_of(lax.axis_index("rep") * plan.feat, LANES)
    return jnp.dot(
        jnp.concatenate(rows, axis=0),
        down_ref[:, pl.ds(first, plan.feat)],
        preferred_element_type=F32,
    )


def down_own_kernel(plan, hidden_ref, down_ref, out_ref):
    out_ref[...] = down_product(plan, hidden_ref, down_ref)


def down_other_kernel(plan, hidden_ref, down_ref, mine_ref, out_ref):
    emit_packed(plan, mine_ref[...] + down_product(plan, hidden_ref, down_ref), out_ref)


def combine_kernel(plan, pick_ref, column_ref, packed_ref, out_ref):
    for part in range(plan.parts):
        blocks = range(part, plan.blocks, plan.parts)
        tables = []
        for block in blocks:
            tiles = [index * plan.blocks + block for index in range(plan.full)]
            if plan.tail:
                tiles.append(plan.full * plan.blocks + block // plan.group)
            tables.append(jnp.concatenate([flat_tile(packed_ref[:, tile]) for tile in tiles], axis=0))
        table = jnp.concatenate(tables, axis=1)
        total = jnp.zeros((plan.tok, table.shape[1]), F32)
        for k in range(plan.choices):
            picked = jnp.dot(pick_ref[k * plan.parts + part], table, preferred_element_type=F32)
            total = total + column_ref[:, k : k + 1] * picked
        for index, block in enumerate(blocks):
            out_ref[:, lane_block(block)] = total[:, lane_block(index)].astype(BF16)


VMEM = pl.BlockSpec(memory_space=pltpu.VMEM)
ANY = pl.BlockSpec(memory_space=pltpu.HBM)


def call(kernel, in_specs, out_shape, flops, moved, limit, scratch=()):
    single = not isinstance(out_shape, (list, tuple))
    return pl.pallas_call(
        kernel,
        in_specs=in_specs,
        out_specs=VMEM if single else [VMEM] * len(out_shape),
        out_shape=out_shape,
        scratch_shapes=list(scratch),
        cost_estimate=pl.CostEstimate(flops=flops, bytes_accessed=moved, transcendentals=0),
        compiler_params=pltpu.CompilerParams(vmem_limit_bytes=limit),
    )


def body(tokens, expert_ids, gate_values, slot_expert, gate_weight, up_weight, down_weight):
    tok, choices = expert_ids.shape
    feat = tokens.shape[1]
    slots = slot_expert.shape[0]
    plan = Plan(tok, choices, feat, slots)
    weights = [gate_weight[0], up_weight[0], down_weight[0]]
    hid = weights[0].shape[1]
    gate_local, up_local, down_local = weights
    swap = [(0, 1), (1, 0)]
    packed_bytes = 2 * slots * plan.tiles * TILE_ROWS * LANES
    half_flops = 4 * plan.rows * feat * hid
    rows_scratch = pltpu.VMEM((plan.rows, feat), BF16)
    packed = jax.ShapeDtypeStruct(plan.packed, BF16)

    slot_row, ids, gates = slot_expert.reshape(1, slots), expert_ids.T, gate_values.T

    down_swapped = lax.ppermute(down_local, "rep", swap)
    warm = call(
        warm_kernel,
        [],
        jax.ShapeDtypeStruct((TILE_ROWS, LANES), F32),
        COVER_FLOPS,
        COVER_BYTES,
        1 * MIB,
    )()
    found = call(
        functools.partial(route_kernel, plan),
        [VMEM] * 3,
        jax.ShapeDtypeStruct((2 * choices, tok), jnp.int32),
        1 << 10,
        1 << 10,
        4 * MIB,
    )(warm, slot_row, ids)
    send = call(
        functools.partial(pack_kernel, plan), [VMEM] * 2, packed, COVER_FLOPS, COVER_BYTES, 8 * MIB
    )(found, tokens)
    arrived = exchange(send, slots)
    partner = lax.ppermute(arrived, "rep", swap)
    acc = call(
        functools.partial(own_kernel, plan),
        [VMEM] * 4,
        jax.ShapeDtypeStruct((plan.rows, 2 * hid), F32),
        1 << 10,
        1 << 10,
        8 * MIB,
        [rows_scratch],
    )(arrived, gate_local, up_local, down_local)
    picks, columns = call(
        functools.partial(select_kernel, plan),
        [VMEM, VMEM],
        [
            jax.ShapeDtypeStruct((choices * plan.parts, tok, plan.wide), BF16),
            jax.ShapeDtypeStruct((tok, choices), F32),
        ],
        1 << 10,
        1 << 10,
        4 * MIB,
    )(found, gates)
    hidden = call(
        functools.partial(other_kernel, plan),
        [VMEM] * 4,
        jax.ShapeDtypeStruct((plan.rows, hid), BF16),
        half_flops,
        packed_bytes + 8 * plan.rows * hid,
        8 * MIB,
        [rows_scratch],
    )(partner, acc, gate_local, up_local)
    received = lax.ppermute(hidden, "rep", swap)
    mine = call(
        functools.partial(down_own_kernel, plan),
        [VMEM] * 2,
        jax.ShapeDtypeStruct((plan.wide, feat), F32),
        2 * plan.wide * hid * feat,
        2 * packed_bytes,
        8 * MIB,
    )(hidden, down_local)
    result = call(
        functools.partial(down_other_kernel, plan),
        [VMEM] * 3,
        packed,
        2 * plan.wide * hid * feat,
        2 * packed_bytes,
        8 * MIB,
    )(received, down_swapped, mine)
    returned = exchange(result, slots)
    return call(
        functools.partial(combine_kernel, plan),
        [VMEM, VMEM, VMEM],
        jax.ShapeDtypeStruct((tok, feat), BF16),
        2 * tok * feat * plan.wide * choices,
        2 * packed_bytes,
        8 * MIB,
    )(picks, columns, returned)


def solution(mesh):
    assert mesh.shape["rep"] == 2
    return jax.shard_map(
        body,
        mesh=mesh,
        in_specs=(
            P(("groups", "ep"), "rep"),
            P(("groups", "ep"), None),
            P(("groups", "ep"), None),
            P(),
            P("ep", None, "rep"),
            P("ep", None, "rep"),
            P("ep", "rep", None),
        ),
        out_specs=P(("groups", "ep"), "rep"),
        check_vma=False,
    )
```

```python
import functools

import jax
import jax.numpy as jnp
from jax import lax
from jax.experimental import pallas as pl
from jax.experimental.pallas import tpu as pltpu
from jax.sharding import PartitionSpec as P


LANES = 128
TILE_ROWS = 4
MIB = 1 << 20
F32 = jnp.float32
BF16 = jnp.bfloat16
COVER_FLOPS = 1 << 34
COVER_BYTES = 1 << 25


class Plan:
    def __init__(self, tok, choices, feat, slots):
        experts = slots // 2
        self.tok, self.choices, self.feat, self.slots = tok, choices, feat, slots
        self.capacity = tok * choices * 5 // (4 * experts)
        assert feat % LANES == 0
        self.blocks = feat // LANES
        self.full = self.capacity // TILE_ROWS
        self.main = self.full * TILE_ROWS
        self.tail = self.capacity - self.main
        self.group = TILE_ROWS // self.tail if self.tail else 0
        self.tail_tiles = -(-self.blocks // self.group) if self.tail else 0
        self.tiles = self.full * self.blocks + self.tail_tiles
        self.main_rows = slots * self.main
        self.tail_rows = slots * self.tail
        self.rows = self.main_rows + self.tail_rows
        self.tail_wide = slots * TILE_ROWS if self.tail else 0
        self.wide = self.main_rows + self.tail_wide
        self.parts = max(1, self.group)
        self.packed = (slots, self.tiles, TILE_ROWS, LANES)


def iota(shape, dim):
    return lax.broadcasted_iota(jnp.int32, shape, dim)


def floor_div(values, divisor):
    return jnp.floor((values.astype(F32) + 0.5) * (1.0 / divisor)).astype(jnp.int32)


def exchange_place(index, members):
    away = index - 1 - members // 2
    away = jnp.where(index == 0, members // 2 - 1, away)
    return jnp.where(away >= 0, 2 * away, -2 * away - 1)


def exchange_order(members):
    away = [index // 2 if index % 2 == 0 else -(index // 2) - 1 for index in range(members)]
    return [(1 + members // 2 + step) % members for step in away]


def exchange(array, members):
    return lax.all_to_all(
        array,
        "ep",
        split_axis=0,
        concat_axis=0,
        tiled=True,
        axis_index_groups=[exchange_order(members)],
    )


def to_column(row):
    size = row.shape[1]
    diagonal = iota((size, size), 0) == iota((size, size), 1)
    return jnp.sum(jnp.where(diagonal, jnp.broadcast_to(row, (size, size)), 0), axis=1, keepdims=True)


def route(plan, member, slot_row, ids):
    slots, tok = plan.slots, plan.tok
    square = (slots, slots)
    col = to_column(slot_row.astype(F32))
    same = jnp.where(col == slot_row.astype(F32), 1.0, 0.0)
    copies = jnp.sum(same, axis=1, keepdims=True)
    rank = jnp.sum(jnp.where(iota(square, 1) < iota(square, 0), same, 0.0), axis=1, keepdims=True)
    want = jnp.zeros((slots, 1), F32)
    for number in (2, 3, 4):
        want = jnp.where(copies == number, lax.rem(member, number).astype(F32), want)
    chosen = rank == want
    line = exchange_place(iota((slots, tok), 0), slots).astype(F32)
    rows = [ids[k : k + 1].astype(F32) for k in range(plan.choices)]
    cols = [to_column(row) for row in rows]
    before = iota((tok, tok), 0) < iota((tok, tok), 1)
    found = []
    for row in rows:
        slot = jnp.sum(jnp.where((row == col) & chosen, line, 0.0), axis=0, keepdims=True)
        earlier = sum(jnp.where((other == row) & before, 1.0, 0.0) for other in cols)
        place = jnp.sum(earlier, axis=0, keepdims=True)
        found.append((slot.astype(jnp.int32), place.astype(jnp.int32)))
    return found


def main_code(plan, slot, place):
    return jnp.where(place < plan.main, slot * plan.main + place, -1)


def table_code(plan, slot, place, part):
    tile = sum((place >= (index + 1) * TILE_ROWS).astype(jnp.int32) for index in range(plan.full))
    inner = place - tile * TILE_ROWS + jnp.where(tile == plan.full, part * plan.tail, 0)
    return (tile * plan.slots + slot) * TILE_ROWS + inner


def tail_code(plan, slot, place, part):
    spot = slot * TILE_ROWS + place - plan.main + part * plan.tail
    return jnp.where(place < plan.main, -1, spot)


def lane_block(index):
    return slice(index * LANES, (index + 1) * LANES)


def warm_kernel(out_ref):
    out_ref[...] = jnp.zeros_like(out_ref)


def read_found(plan, found_ref):
    lines = [found_ref[index : index + 1] for index in range(2 * plan.choices)]
    return list(zip(lines[: plan.choices], lines[plan.choices :], strict=True))


def route_kernel(plan, warm_ref, slot_ref, ids_ref, found_ref):
    found = route(plan, lax.axis_index("ep"), slot_ref[...], ids_ref[...])
    for k, (slot, place) in enumerate(found):
        found_ref[k : k + 1] = slot
        found_ref[plan.choices + k : plan.choices + k + 1] = place


def pack_kernel(plan, found_ref, tokens_ref, send_ref):
    found = read_found(plan, found_ref)
    if plan.full:
        line = iota((plan.main_rows, plan.tok), 0)
        hot = sum(jnp.where(line == main_code(plan, *pair), 1.0, 0.0) for pair in found)
        main = jnp.dot(hot.astype(BF16), tokens_ref[...], preferred_element_type=F32)
        for block in range(plan.blocks):
            tile = main[:, lane_block(block)].reshape(plan.slots, plan.full, TILE_ROWS, LANES)
            for index in range(plan.full):
                send_ref[:, index * plan.blocks + block] = tile[:, index].astype(BF16)
    if plan.tail:
        line = iota((plan.tail_wide, plan.tok * plan.group), 0)
        hot = jnp.zeros(line.shape, F32)
        for pair in found:
            codes = [tail_code(plan, *pair, part) for part in range(plan.group)]
            hot += jnp.where(line == jnp.concatenate(codes, axis=1), 1.0, 0.0)
        hot = hot.astype(BF16)
        for index in range(plan.tail_tiles):
            stack = []
            for part in range(plan.group):
                block = index * plan.group + part
                if block < plan.blocks:
                    stack.append(tokens_ref[:, lane_block(block)])
                else:
                    stack.append(jnp.zeros((plan.tok, LANES), BF16))
            tile = jnp.dot(hot, jnp.concatenate(stack, axis=0), preferred_element_type=F32)
            send_ref[:, plan.full * plan.blocks + index] = tile.reshape(
                plan.slots, TILE_ROWS, LANES
            ).astype(BF16)


def select_kernel(plan, found_ref, gates_ref, pick_ref, column_ref):
    lane = iota((plan.tok, plan.wide), 1).astype(F32)
    for k, (slot, place) in enumerate(read_found(plan, found_ref)):
        column_ref[:, k : k + 1] = to_column(gates_ref[k : k + 1])
        for part in range(plan.parts):
            code = table_code(plan, slot, place, part)
            pick = jnp.where(to_column(code.astype(F32)) == lane, 1.0, 0.0)
            pick_ref[k * plan.parts + part] = pick.astype(BF16)


def flat_tile(tile):
    return tile.reshape(-1, LANES)


def unpack_rows(plan, packed_ref, rows_ref):
    for block in range(plan.blocks):
        for index in range(plan.full):
            tile = packed_ref[:, index * plan.blocks + block]
            if plan.full == 1:
                rows_ref[0 : plan.main_rows, lane_block(block)] = flat_tile(tile)
            else:
                for sender in range(plan.slots):
                    first = sender * plan.main + index * TILE_ROWS
                    rows_ref[first : first + TILE_ROWS, lane_block(block)] = tile[sender]
    if plan.tail:
        shape = (plan.group * plan.tail_rows, plan.tail_wide)
        line = iota(shape, 0)
        part = floor_div(line, plan.tail_rows)
        inner = line - part * plan.tail_rows
        sender = floor_div(inner, plan.tail)
        spot = sender * TILE_ROWS + part * plan.tail + inner - sender * plan.tail
        hot = jnp.where(spot == iota(shape, 1), 1.0, 0.0).astype(BF16)
        for index in range(plan.tail_tiles):
            tile = flat_tile(packed_ref[:, plan.full * plan.blocks + index])
            moved = jnp.dot(hot, tile, preferred_element_type=F32).astype(BF16)
            for part in range(plan.group):
                block = index * plan.group + part
                if block < plan.blocks:
                    rows_ref[plan.main_rows : plan.rows, lane_block(block)] = moved[
                        part * plan.tail_rows : (part + 1) * plan.tail_rows
                    ]


def own_kernel(plan, packed_ref, gate_ref, up_ref, down_ref, acc_ref, rows_ref):
    unpack_rows(plan, packed_ref, rows_ref)
    first = pl.multiple_of(lax.axis_index("rep") * plan.feat, LANES)
    hid = gate_ref.shape[1]
    rows = rows_ref[...]
    acc_ref[:, :hid] = jnp.dot(
        rows, gate_ref[pl.ds(first, plan.feat), :], preferred_element_type=F32
    )
    acc_ref[:, hid:] = jnp.dot(
        rows, up_ref[pl.ds(first, plan.feat), :], preferred_element_type=F32
    )


def emit_packed(plan, product, out_ref):
    for block in range(plan.blocks):
        tile = product[: plan.main_rows, lane_block(block)].reshape(
            plan.slots, plan.full, TILE_ROWS, LANES
        )
        for index in range(plan.full):
            out_ref[:, index * plan.blocks + block] = tile[:, index].astype(out_ref.dtype)
    for index in range(plan.tail_tiles):
        parts = []
        for part in range(plan.group):
            block = index * plan.group + part
            if block < plan.blocks:
                piece = product[plan.main_rows :, lane_block(block)]
                parts.append(piece.reshape(plan.slots, plan.tail, LANES))
        while len(parts) * plan.tail < TILE_ROWS:
            parts.append(jnp.zeros((plan.slots, min(plan.tail, TILE_ROWS - len(parts) * plan.tail), LANES), F32))
        tile = jnp.concatenate(parts, axis=1)
        out_ref[:, plan.full * plan.blocks + index] = tile.astype(out_ref.dtype)


def other_kernel(plan, packed_ref, acc_ref, gate_ref, up_ref, hidden_ref, rows_ref):
    unpack_rows(plan, packed_ref, rows_ref)
    first = pl.multiple_of((1 - lax.axis_index("rep")) * plan.feat, LANES)
    hid = gate_ref.shape[1]
    rows = rows_ref[...]
    gate = acc_ref[:, :hid] + jnp.dot(
        rows, gate_ref[pl.ds(first, plan.feat), :], preferred_element_type=F32
    )
    up = acc_ref[:, hid:] + jnp.dot(
        rows, up_ref[pl.ds(first, plan.feat), :], preferred_element_type=F32
    )
    hidden_ref[...] = (gate / (1.0 + jnp.exp(-gate)) * up).astype(BF16)


def down_product(plan, hidden_ref, down_ref):
    first = pl.multiple_of(lax.axis_index("rep") * plan.feat, LANES)
    return jnp.dot(
        hidden_ref[...], down_ref[:, pl.ds(first, plan.feat)], preferred_element_type=F32
    )


def down_own_kernel(plan, hidden_ref, down_ref, out_ref):
    out_ref[...] = down_product(plan, hidden_ref, down_ref)


def down_other_kernel(plan, hidden_ref, down_ref, mine_ref, out_ref):
    emit_packed(plan, mine_ref[...] + down_product(plan, hidden_ref, down_ref), out_ref)


def combine_kernel(plan, pick_ref, column_ref, packed_ref, out_ref):
    for part in range(plan.parts):
        blocks = range(part, plan.blocks, plan.parts)
        tables = []
        for block in blocks:
            tiles = [index * plan.blocks + block for index in range(plan.full)]
            if plan.tail:
                tiles.append(plan.full * plan.blocks + block // plan.group)
            tables.append(jnp.concatenate([flat_tile(packed_ref[:, tile]) for tile in tiles], axis=0))
        table = jnp.concatenate(tables, axis=1)
        total = jnp.zeros((plan.tok, table.shape[1]), F32)
        for k in range(plan.choices):
            picked = jnp.dot(pick_ref[k * plan.parts + part], table, preferred_element_type=F32)
            total = total + column_ref[:, k : k + 1] * picked
        for index, block in enumerate(blocks):
            out_ref[:, lane_block(block)] = total[:, lane_block(index)].astype(BF16)


VMEM = pl.BlockSpec(memory_space=pltpu.VMEM)
ANY = pl.BlockSpec(memory_space=pltpu.HBM)


def call(kernel, in_specs, out_shape, flops, moved, limit, scratch=()):
    single = not isinstance(out_shape, (list, tuple))
    return pl.pallas_call(
        kernel,
        in_specs=in_specs,
        out_specs=VMEM if single else [VMEM] * len(out_shape),
        out_shape=out_shape,
        scratch_shapes=list(scratch),
        cost_estimate=pl.CostEstimate(flops=flops, bytes_accessed=moved, transcendentals=0),
        compiler_params=pltpu.CompilerParams(vmem_limit_bytes=limit),
    )


def body(tokens, expert_ids, gate_values, slot_expert, gate_weight, up_weight, down_weight):
    tok, choices = expert_ids.shape
    feat = tokens.shape[1]
    slots = slot_expert.shape[0]
    plan = Plan(tok, choices, feat, slots)
    weights = [gate_weight[0], up_weight[0], down_weight[0]]
    hid = weights[0].shape[1]
    gate_local, up_local, down_local = weights
    swap = [(0, 1), (1, 0)]
    packed_bytes = 2 * slots * plan.tiles * TILE_ROWS * LANES
    half_flops = 4 * plan.rows * feat * hid
    rows_scratch = pltpu.VMEM((plan.rows, feat), BF16)
    packed = jax.ShapeDtypeStruct(plan.packed, BF16)

    slot_row, ids, gates = slot_expert.reshape(1, slots), expert_ids.T, gate_values.T

    down_swapped = lax.ppermute(down_local, "rep", swap)
    warm = call(
        warm_kernel,
        [],
        jax.ShapeDtypeStruct((TILE_ROWS, LANES), F32),
        COVER_FLOPS,
        COVER_BYTES,
        1 * MIB,
    )()
    found = call(
        functools.partial(route_kernel, plan),
        [VMEM] * 3,
        jax.ShapeDtypeStruct((2 * choices, tok), jnp.int32),
        1 << 10,
        1 << 10,
        4 * MIB,
    )(warm, slot_row, ids)
    send = call(
        functools.partial(pack_kernel, plan), [VMEM] * 2, packed, COVER_FLOPS, COVER_BYTES, 8 * MIB
    )(found, tokens)
    arrived = exchange(send, slots)
    partner = lax.ppermute(arrived, "rep", swap)
    acc = call(
        functools.partial(own_kernel, plan),
        [VMEM] * 4,
        jax.ShapeDtypeStruct((plan.rows, 2 * hid), F32),
        1 << 10,
        1 << 10,
        8 * MIB,
        [rows_scratch],
    )(arrived, gate_local, up_local, down_local)
    picks, columns = call(
        functools.partial(select_kernel, plan),
        [VMEM, VMEM],
        [
            jax.ShapeDtypeStruct((choices * plan.parts, tok, plan.wide), BF16),
            jax.ShapeDtypeStruct((tok, choices), F32),
        ],
        1 << 10,
        1 << 10,
        4 * MIB,
    )(found, gates)
    hidden = call(
        functools.partial(other_kernel, plan),
        [VMEM] * 4,
        jax.ShapeDtypeStruct((plan.rows, hid), BF16),
        half_flops,
        packed_bytes + 8 * plan.rows * hid,
        8 * MIB,
        [rows_scratch],
    )(partner, acc, gate_local, up_local)
    received = lax.ppermute(hidden, "rep", swap)
    mine = call(
        functools.partial(down_own_kernel, plan),
        [VMEM] * 2,
        jax.ShapeDtypeStruct((plan.rows, feat), F32),
        2 * plan.wide * hid * feat,
        2 * packed_bytes,
        8 * MIB,
    )(hidden, down_local)
    result = call(
        functools.partial(down_other_kernel, plan),
        [VMEM] * 3,
        packed,
        2 * plan.wide * hid * feat,
        2 * packed_bytes,
        8 * MIB,
    )(received, down_swapped, mine)
    returned = exchange(result, slots)
    return call(
        functools.partial(combine_kernel, plan),
        [VMEM, VMEM, VMEM],
        jax.ShapeDtypeStruct((tok, feat), BF16),
        2 * tok * feat * plan.wide * choices,
        2 * packed_bytes,
        8 * MIB,
    )(picks, columns, returned)


def solution(mesh):
    assert mesh.shape["rep"] == 2
    return jax.shard_map(
        body,
        mesh=mesh,
        in_specs=(
            P(("groups", "ep"), "rep"),
            P(("groups", "ep"), None),
            P(("groups", "ep"), None),
            P(),
            P("ep", None, "rep"),
            P("ep", None, "rep"),
            P("ep", "rep", None),
        ),
        out_specs=P(("groups", "ep"), "rep"),
        check_vma=False,
    )
```

```python
import functools

import jax
import jax.numpy as jnp
from jax import lax
from jax.experimental import pallas as pl
from jax.experimental.pallas import tpu as pltpu
from jax.sharding import PartitionSpec as P


LANES = 128
TILE_ROWS = 4
MIB = 1 << 20
F32 = jnp.float32
BF16 = jnp.bfloat16
COVER_FLOPS = 1 << 34
COVER_BYTES = 1 << 25


class Plan:
    def __init__(self, tok, choices, feat, slots):
        experts = slots // 2
        self.tok, self.choices, self.feat, self.slots = tok, choices, feat, slots
        self.capacity = tok * choices * 5 // (4 * experts)
        assert feat % LANES == 0
        self.blocks = feat // LANES
        self.full = self.capacity // TILE_ROWS
        self.main = self.full * TILE_ROWS
        self.tail = self.capacity - self.main
        self.group = TILE_ROWS // self.tail if self.tail else 0
        self.tail_tiles = -(-self.blocks // self.group) if self.tail else 0
        self.tiles = self.full * self.blocks + self.tail_tiles
        self.main_rows = slots * self.main
        self.tail_rows = slots * self.tail
        self.rows = self.main_rows + self.tail_rows
        self.tail_wide = slots * TILE_ROWS if self.tail else 0
        self.wide = self.main_rows + self.tail_wide
        self.parts = max(1, self.group)
        self.packed = (slots, self.tiles, TILE_ROWS, LANES)


def iota(shape, dim):
    return lax.broadcasted_iota(jnp.int32, shape, dim)


def exchange_place(index, members):
    away = index - 1 - members // 2
    away = jnp.where(index == 0, members // 2 - 1, away)
    return jnp.where(away >= 0, 2 * away, -2 * away - 1)


def exchange_order(members):
    away = [index // 2 if index % 2 == 0 else -(index // 2) - 1 for index in range(members)]
    return [(1 + members // 2 + step) % members for step in away]


def exchange(array, members):
    return lax.all_to_all(
        array,
        "ep",
        split_axis=0,
        concat_axis=0,
        tiled=True,
        axis_index_groups=[exchange_order(members)],
    )


def to_column(row):
    size = row.shape[1]
    diagonal = iota((size, size), 0) == iota((size, size), 1)
    return jnp.sum(jnp.where(diagonal, jnp.broadcast_to(row, (size, size)), 0), axis=1, keepdims=True)


def route(plan, member, slot_row, ids):
    slots, tok = plan.slots, plan.tok
    square = (slots, slots)
    col = to_column(slot_row.astype(F32))
    same = jnp.where(col == slot_row.astype(F32), 1.0, 0.0)
    copies = jnp.sum(same, axis=1, keepdims=True)
    rank = jnp.sum(jnp.where(iota(square, 1) < iota(square, 0), same, 0.0), axis=1, keepdims=True)
    want = jnp.zeros((slots, 1), F32)
    for number in (2, 3, 4):
        want = jnp.where(copies == number, lax.rem(member, number).astype(F32), want)
    chosen = rank == want
    line = exchange_place(iota((slots, tok), 0), slots).astype(F32)
    rows = [ids[k : k + 1].astype(F32) for k in range(plan.choices)]
    cols = [to_column(row) for row in rows]
    before = iota((tok, tok), 0) < iota((tok, tok), 1)
    found = []
    for row in rows:
        slot = jnp.sum(jnp.where((row == col) & chosen, line, 0.0), axis=0, keepdims=True)
        earlier = sum(jnp.where((other == row) & before, 1.0, 0.0) for other in cols)
        place = jnp.sum(earlier, axis=0, keepdims=True)
        found.append((slot.astype(jnp.int32), place.astype(jnp.int32)))
    return found


def main_code(plan, slot, place):
    return jnp.where(place < plan.main, slot * plan.main + place, -1)


def table_code(plan, slot, place, part):
    tile = sum((place >= (index + 1) * TILE_ROWS).astype(jnp.int32) for index in range(plan.full))
    inner = place - tile * TILE_ROWS + jnp.where(tile == plan.full, part * plan.tail, 0)
    return (tile * plan.slots + slot) * TILE_ROWS + inner


def tail_code(plan, slot, place, part):
    spot = slot * TILE_ROWS + place - plan.main + part * plan.tail
    return jnp.where(place < plan.main, -1, spot)


def lane_block(index):
    return slice(index * LANES, (index + 1) * LANES)


def warm_kernel(out_ref):
    out_ref[...] = jnp.zeros_like(out_ref)


def read_found(plan, found_ref):
    lines = [found_ref[index : index + 1] for index in range(2 * plan.choices)]
    return list(zip(lines[: plan.choices], lines[plan.choices :], strict=True))


def route_kernel(plan, warm_ref, slot_ref, ids_ref, found_ref):
    found = route(plan, lax.axis_index("ep"), slot_ref[...], ids_ref[...])
    for k, (slot, place) in enumerate(found):
        found_ref[k : k + 1] = slot
        found_ref[plan.choices + k : plan.choices + k + 1] = place


def pack_kernel(plan, found_ref, tokens_ref, send_ref):
    found = read_found(plan, found_ref)
    if plan.full:
        line = iota((plan.main_rows, plan.tok), 0)
        hot = sum(jnp.where(line == main_code(plan, *pair), 1.0, 0.0) for pair in found)
        main = jnp.dot(hot.astype(BF16), tokens_ref[...], preferred_element_type=F32)
        for block in range(plan.blocks):
            tile = main[:, lane_block(block)].reshape(plan.slots, plan.full, TILE_ROWS, LANES)
            for index in range(plan.full):
                send_ref[:, index * plan.blocks + block] = tile[:, index].astype(BF16)
    if plan.tail:
        line = iota((plan.tail_wide, plan.tok * plan.group), 0)
        hot = jnp.zeros(line.shape, F32)
        for pair in found:
            codes = [tail_code(plan, *pair, part) for part in range(plan.group)]
            hot += jnp.where(line == jnp.concatenate(codes, axis=1), 1.0, 0.0)
        hot = hot.astype(BF16)
        for index in range(plan.tail_tiles):
            stack = []
            for part in range(plan.group):
                block = index * plan.group + part
                if block < plan.blocks:
                    stack.append(tokens_ref[:, lane_block(block)])
                else:
                    stack.append(jnp.zeros((plan.tok, LANES), BF16))
            tile = jnp.dot(hot, jnp.concatenate(stack, axis=0), preferred_element_type=F32)
            send_ref[:, plan.full * plan.blocks + index] = tile.reshape(
                plan.slots, TILE_ROWS, LANES
            ).astype(BF16)


def select_kernel(plan, found_ref, gates_ref, pick_ref, column_ref):
    lane = iota((plan.tok, plan.wide), 1).astype(F32)
    for k, (slot, place) in enumerate(read_found(plan, found_ref)):
        column_ref[:, k : k + 1] = to_column(gates_ref[k : k + 1])
        for part in range(plan.parts):
            code = table_code(plan, slot, place, part)
            pick = jnp.where(to_column(code.astype(F32)) == lane, 1.0, 0.0)
            pick_ref[k * plan.parts + part] = pick.astype(BF16)


def flat_tile(tile):
    return tile.reshape(-1, LANES)


def unpack_rows(plan, packed_ref, rows_ref):
    for block in range(plan.blocks):
        for index in range(plan.full):
            tile = packed_ref[:, index * plan.blocks + block]
            if plan.full == 1:
                rows_ref[0 : plan.main_rows, lane_block(block)] = flat_tile(tile)
            else:
                for sender in range(plan.slots):
                    first = sender * plan.main + index * TILE_ROWS
                    rows_ref[first : first + TILE_ROWS, lane_block(block)] = tile[sender]
    for index in range(plan.tail_tiles):
        tile = packed_ref[:, plan.full * plan.blocks + index]
        for part in range(plan.group):
            block = index * plan.group + part
            if block < plan.blocks:
                piece = tile.astype(F32)[:, part * plan.tail : (part + 1) * plan.tail]
                piece = piece.reshape(plan.tail_rows, LANES).astype(BF16)
                rows_ref[plan.main_rows : plan.rows, lane_block(block)] = piece


def own_kernel(plan, packed_ref, gate_ref, up_ref, down_ref, acc_ref, rows_ref):
    unpack_rows(plan, packed_ref, rows_ref)
    first = pl.multiple_of(lax.axis_index("rep") * plan.feat, LANES)
    hid = gate_ref.shape[1]
    rows = rows_ref[...]
    acc_ref[:, :hid] = jnp.dot(
        rows, gate_ref[pl.ds(first, plan.feat), :], preferred_element_type=F32
    )
    acc_ref[:, hid:] = jnp.dot(
        rows, up_ref[pl.ds(first, plan.feat), :], preferred_element_type=F32
    )


def emit_packed(plan, product, out_ref):
    for block in range(plan.blocks):
        tile = product[: plan.main_rows, lane_block(block)].reshape(
            plan.slots, plan.full, TILE_ROWS, LANES
        )
        for index in range(plan.full):
            out_ref[:, index * plan.blocks + block] = tile[:, index].astype(out_ref.dtype)
    for index in range(plan.tail_tiles):
        parts = []
        for part in range(plan.group):
            block = index * plan.group + part
            if block < plan.blocks:
                piece = product[plan.main_rows :, lane_block(block)]
                parts.append(piece.reshape(plan.slots, plan.tail, LANES))
        while len(parts) * plan.tail < TILE_ROWS:
            parts.append(jnp.zeros((plan.slots, min(plan.tail, TILE_ROWS - len(parts) * plan.tail), LANES), F32))
        tile = jnp.concatenate(parts, axis=1)
        out_ref[:, plan.full * plan.blocks + index] = tile.astype(out_ref.dtype)


def other_kernel(plan, packed_ref, acc_ref, gate_ref, up_ref, hidden_ref, rows_ref):
    unpack_rows(plan, packed_ref, rows_ref)
    first = pl.multiple_of((1 - lax.axis_index("rep")) * plan.feat, LANES)
    hid = gate_ref.shape[1]
    rows = rows_ref[...]
    gate = acc_ref[:, :hid] + jnp.dot(
        rows, gate_ref[pl.ds(first, plan.feat), :], preferred_element_type=F32
    )
    up = acc_ref[:, hid:] + jnp.dot(
        rows, up_ref[pl.ds(first, plan.feat), :], preferred_element_type=F32
    )
    hidden_ref[...] = (gate / (1.0 + jnp.exp(-gate)) * up).astype(BF16)


def down_product(plan, hidden_ref, down_ref):
    first = pl.multiple_of(lax.axis_index("rep") * plan.feat, LANES)
    return jnp.dot(
        hidden_ref[...], down_ref[:, pl.ds(first, plan.feat)], preferred_element_type=F32
    )


def down_own_kernel(plan, hidden_ref, down_ref, out_ref):
    out_ref[...] = down_product(plan, hidden_ref, down_ref)


def down_other_kernel(plan, hidden_ref, down_ref, mine_ref, out_ref):
    emit_packed(plan, mine_ref[...] + down_product(plan, hidden_ref, down_ref), out_ref)


def combine_kernel(plan, pick_ref, column_ref, packed_ref, out_ref):
    for part in range(plan.parts):
        blocks = range(part, plan.blocks, plan.parts)
        tables = []
        for block in blocks:
            tiles = [index * plan.blocks + block for index in range(plan.full)]
            if plan.tail:
                tiles.append(plan.full * plan.blocks + block // plan.group)
            tables.append(jnp.concatenate([flat_tile(packed_ref[:, tile]) for tile in tiles], axis=0))
        table = jnp.concatenate(tables, axis=1)
        total = jnp.zeros((plan.tok, table.shape[1]), F32)
        for k in range(plan.choices):
            picked = jnp.dot(pick_ref[k * plan.parts + part], table, preferred_element_type=F32)
            total = total + column_ref[:, k : k + 1] * picked
        for index, block in enumerate(blocks):
            out_ref[:, lane_block(block)] = total[:, lane_block(index)].astype(BF16)


VMEM = pl.BlockSpec(memory_space=pltpu.VMEM)
ANY = pl.BlockSpec(memory_space=pltpu.HBM)


def call(kernel, in_specs, out_shape, flops, moved, limit, scratch=()):
    single = not isinstance(out_shape, (list, tuple))
    return pl.pallas_call(
        kernel,
        in_specs=in_specs,
        out_specs=VMEM if single else [VMEM] * len(out_shape),
        out_shape=out_shape,
        scratch_shapes=list(scratch),
        cost_estimate=pl.CostEstimate(flops=flops, bytes_accessed=moved, transcendentals=0),
        compiler_params=pltpu.CompilerParams(vmem_limit_bytes=limit),
    )


def body(tokens, expert_ids, gate_values, slot_expert, gate_weight, up_weight, down_weight):
    tok, choices = expert_ids.shape
    feat = tokens.shape[1]
    slots = slot_expert.shape[0]
    plan = Plan(tok, choices, feat, slots)
    weights = [gate_weight[0], up_weight[0], down_weight[0]]
    hid = weights[0].shape[1]
    gate_local, up_local, down_local = weights
    swap = [(0, 1), (1, 0)]
    packed_bytes = 2 * slots * plan.tiles * TILE_ROWS * LANES
    half_flops = 4 * plan.rows * feat * hid
    rows_scratch = pltpu.VMEM((plan.rows, feat), BF16)
    packed = jax.ShapeDtypeStruct(plan.packed, BF16)

    slot_row, ids, gates = slot_expert.reshape(1, slots), expert_ids.T, gate_values.T

    down_swapped = lax.ppermute(down_local, "rep", swap)
    warm = call(
        warm_kernel,
        [],
        jax.ShapeDtypeStruct((TILE_ROWS, LANES), F32),
        COVER_FLOPS,
        COVER_BYTES,
        1 * MIB,
    )()
    found = call(
        functools.partial(route_kernel, plan),
        [VMEM] * 3,
        jax.ShapeDtypeStruct((2 * choices, tok), jnp.int32),
        1 << 10,
        1 << 10,
        4 * MIB,
    )(warm, slot_row, ids)
    send = call(
        functools.partial(pack_kernel, plan), [VMEM] * 2, packed, COVER_FLOPS, COVER_BYTES, 8 * MIB
    )(found, tokens)
    arrived = exchange(send, slots)
    partner = lax.ppermute(arrived, "rep", swap)
    acc = call(
        functools.partial(own_kernel, plan),
        [VMEM] * 4,
        jax.ShapeDtypeStruct((plan.rows, 2 * hid), F32),
        1 << 10,
        1 << 10,
        8 * MIB,
        [rows_scratch],
    )(arrived, gate_local, up_local, down_local)
    picks, columns = call(
        functools.partial(select_kernel, plan),
        [VMEM, VMEM],
        [
            jax.ShapeDtypeStruct((choices * plan.parts, tok, plan.wide), BF16),
            jax.ShapeDtypeStruct((tok, choices), F32),
        ],
        1 << 10,
        1 << 10,
        4 * MIB,
    )(found, gates)
    hidden = call(
        functools.partial(other_kernel, plan),
        [VMEM] * 4,
        jax.ShapeDtypeStruct((plan.rows, hid), BF16),
        half_flops,
        packed_bytes + 8 * plan.rows * hid,
        8 * MIB,
        [rows_scratch],
    )(partner, acc, gate_local, up_local)
    received = lax.ppermute(hidden, "rep", swap)
    mine = call(
        functools.partial(down_own_kernel, plan),
        [VMEM] * 2,
        jax.ShapeDtypeStruct((plan.rows, feat), F32),
        2 * plan.wide * hid * feat,
        2 * packed_bytes,
        8 * MIB,
    )(hidden, down_local)
    result = call(
        functools.partial(down_other_kernel, plan),
        [VMEM] * 3,
        packed,
        2 * plan.wide * hid * feat,
        2 * packed_bytes,
        8 * MIB,
    )(received, down_swapped, mine)
    returned = exchange(result, slots)
    return call(
        functools.partial(combine_kernel, plan),
        [VMEM, VMEM, VMEM],
        jax.ShapeDtypeStruct((tok, feat), BF16),
        2 * tok * feat * plan.wide * choices,
        2 * packed_bytes,
        8 * MIB,
    )(picks, columns, returned)


def solution(mesh):
    assert mesh.shape["rep"] == 2
    return jax.shard_map(
        body,
        mesh=mesh,
        in_specs=(
            P(("groups", "ep"), "rep"),
            P(("groups", "ep"), None),
            P(("groups", "ep"), None),
            P(),
            P("ep", None, "rep"),
            P("ep", None, "rep"),
            P("ep", "rep", None),
        ),
        out_specs=P(("groups", "ep"), "rep"),
        check_vma=False,
    )
```

```python
import functools

import jax
import jax.numpy as jnp
from jax import lax
from jax.experimental import pallas as pl
from jax.experimental.pallas import tpu as pltpu
from jax.sharding import PartitionSpec as P


LANES = 128
TILE_ROWS = 4
MIB = 1 << 20
F32 = jnp.float32
BF16 = jnp.bfloat16
COVER_FLOPS = 1 << 34
COVER_BYTES = 1 << 25


class Plan:
    def __init__(self, tok, choices, feat, slots):
        experts = slots // 2
        self.tok, self.choices, self.feat, self.slots = tok, choices, feat, slots
        self.capacity = tok * choices * 5 // (4 * experts)
        assert feat % LANES == 0
        self.blocks = feat // LANES
        self.full = self.capacity // TILE_ROWS
        self.main = self.full * TILE_ROWS
        self.tail = self.capacity - self.main
        self.group = TILE_ROWS // self.tail if self.tail else 0
        self.tail_tiles = -(-self.blocks // self.group) if self.tail else 0
        self.tiles = self.full * self.blocks + self.tail_tiles
        self.main_rows = slots * self.main
        self.tail_rows = slots * self.tail
        self.rows = self.main_rows + self.tail_rows
        self.tail_wide = slots * TILE_ROWS if self.tail else 0
        self.wide = self.main_rows + self.tail_wide
        self.parts = max(1, self.group)
        self.packed = (slots, self.tiles, TILE_ROWS, LANES)


def iota(shape, dim):
    return lax.broadcasted_iota(jnp.int32, shape, dim)


def exchange_place(index, members):
    away = index - 1 - members // 2
    away = jnp.where(index == 0, members // 2 - 1, away)
    return jnp.where(away >= 0, 2 * away, -2 * away - 1)


def exchange_order(members):
    away = [index // 2 if index % 2 == 0 else -(index // 2) - 1 for index in range(members)]
    return [(1 + members // 2 + step) % members for step in away]


def exchange(array, members):
    return lax.all_to_all(
        array,
        "ep",
        split_axis=0,
        concat_axis=0,
        tiled=True,
        axis_index_groups=[exchange_order(members)],
    )


def to_column(row):
    size = row.shape[1]
    diagonal = iota((size, size), 0) == iota((size, size), 1)
    return jnp.sum(jnp.where(diagonal, jnp.broadcast_to(row, (size, size)), 0), axis=1, keepdims=True)


def route(plan, member, slot_row, ids):
    slots, tok = plan.slots, plan.tok
    square = (slots, slots)
    col = to_column(slot_row.astype(F32))
    same = jnp.where(col == slot_row.astype(F32), 1.0, 0.0)
    copies = jnp.sum(same, axis=1, keepdims=True)
    rank = jnp.sum(jnp.where(iota(square, 1) < iota(square, 0), same, 0.0), axis=1, keepdims=True)
    want = jnp.zeros((slots, 1), F32)
    for number in (2, 3, 4):
        want = jnp.where(copies == number, lax.rem(member, number).astype(F32), want)
    chosen = rank == want
    line = exchange_place(iota((slots, tok), 0), slots).astype(F32)
    rows = [ids[k : k + 1].astype(F32) for k in range(plan.choices)]
    cols = [to_column(row) for row in rows]
    before = iota((tok, tok), 0) < iota((tok, tok), 1)
    found = []
    for row in rows:
        slot = jnp.sum(jnp.where((row == col) & chosen, line, 0.0), axis=0, keepdims=True)
        earlier = sum(jnp.where((other == row) & before, 1.0, 0.0) for other in cols)
        place = jnp.sum(earlier, axis=0, keepdims=True)
        found.append((slot.astype(jnp.int32), place.astype(jnp.int32)))
    return found


def main_code(plan, slot, place):
    return jnp.where(place < plan.main, slot * plan.main + place, -1)


def table_code(plan, slot, place, part):
    tile = sum((place >= (index + 1) * TILE_ROWS).astype(jnp.int32) for index in range(plan.full))
    inner = place - tile * TILE_ROWS + jnp.where(tile == plan.full, part * plan.tail, 0)
    return (tile * plan.slots + slot) * TILE_ROWS + inner


def tail_code(plan, slot, place, part):
    spot = slot * TILE_ROWS + place - plan.main + part * plan.tail
    return jnp.where(place < plan.main, -1, spot)


def lane_block(index):
    return slice(index * LANES, (index + 1) * LANES)


def warm_kernel(out_ref):
    out_ref[...] = jnp.zeros_like(out_ref)


def read_found(plan, found_ref):
    lines = [found_ref[index : index + 1] for index in range(2 * plan.choices)]
    return list(zip(lines[: plan.choices], lines[plan.choices :], strict=True))


def route_kernel(plan, warm_ref, slot_ref, ids_ref, found_ref):
    found = route(plan, lax.axis_index("ep"), slot_ref[...], ids_ref[...])
    for k, (slot, place) in enumerate(found):
        found_ref[k : k + 1] = slot
        found_ref[plan.choices + k : plan.choices + k + 1] = place


def pack_kernel(plan, found_ref, tokens_ref, send_ref):
    found = read_found(plan, found_ref)
    if plan.full:
        line = iota((plan.main_rows, plan.tok), 0)
        hot = sum(jnp.where(line == main_code(plan, *pair), 1.0, 0.0) for pair in found)
        main = jnp.dot(hot.astype(BF16), tokens_ref[...], preferred_element_type=F32)
        for block in range(plan.blocks):
            tile = main[:, lane_block(block)].reshape(plan.slots, plan.full, TILE_ROWS, LANES)
            for index in range(plan.full):
                send_ref[:, index * plan.blocks + block] = tile[:, index].astype(BF16)
    if plan.tail:
        line = iota((plan.tail_wide, plan.tok * plan.group), 0)
        hot = jnp.zeros(line.shape, F32)
        for pair in found:
            codes = [tail_code(plan, *pair, part) for part in range(plan.group)]
            hot += jnp.where(line == jnp.concatenate(codes, axis=1), 1.0, 0.0)
        hot = hot.astype(BF16)
        for index in range(plan.tail_tiles):
            stack = []
            for part in range(plan.group):
                block = index * plan.group + part
                if block < plan.blocks:
                    stack.append(tokens_ref[:, lane_block(block)])
                else:
                    stack.append(jnp.zeros((plan.tok, LANES), BF16))
            tile = jnp.dot(hot, jnp.concatenate(stack, axis=0), preferred_element_type=F32)
            send_ref[:, plan.full * plan.blocks + index] = tile.reshape(
                plan.slots, TILE_ROWS, LANES
            ).astype(BF16)


def select_kernel(plan, found_ref, gates_ref, pick_ref, column_ref):
    lane = iota((plan.tok, plan.wide), 1).astype(F32)
    for k, (slot, place) in enumerate(read_found(plan, found_ref)):
        column_ref[:, k : k + 1] = to_column(gates_ref[k : k + 1])
        for part in range(plan.parts):
            code = table_code(plan, slot, place, part)
            pick = jnp.where(to_column(code.astype(F32)) == lane, 1.0, 0.0)
            pick_ref[k * plan.parts + part] = pick.astype(BF16)


def flat_tile(tile):
    return tile.reshape(-1, LANES)


def unpack_rows(plan, packed_ref, rows_ref):
    for block in range(plan.blocks):
        for index in range(plan.full):
            tile = packed_ref[:, index * plan.blocks + block]
            if plan.full == 1:
                rows_ref[0 : plan.main_rows, lane_block(block)] = flat_tile(tile)
            else:
                for sender in range(plan.slots):
                    first = sender * plan.main + index * TILE_ROWS
                    rows_ref[first : first + TILE_ROWS, lane_block(block)] = tile[sender]
    for index in range(plan.tail_tiles):
        tile = packed_ref[:, plan.full * plan.blocks + index]
        for part in range(plan.group):
            block = index * plan.group + part
            if block < plan.blocks:
                piece = tile.astype(F32)[:, part * plan.tail : (part + 1) * plan.tail]
                piece = piece.reshape(plan.tail_rows, LANES).astype(BF16)
                rows_ref[plan.main_rows : plan.rows, lane_block(block)] = piece


def own_kernel(plan, packed_ref, gate_ref, up_ref, down_ref, acc_ref, rows_ref):
    unpack_rows(plan, packed_ref, rows_ref)
    first = pl.multiple_of(lax.axis_index("rep") * plan.feat, LANES)
    hid = gate_ref.shape[1]
    rows = rows_ref[...]
    acc_ref[:, :hid] = jnp.dot(
        rows, gate_ref[pl.ds(first, plan.feat), :], preferred_element_type=F32
    )
    acc_ref[:, hid:] = jnp.dot(
        rows, up_ref[pl.ds(first, plan.feat), :], preferred_element_type=F32
    )


def emit_packed(plan, product, out_ref):
    for block in range(plan.blocks):
        tile = product[: plan.main_rows, lane_block(block)].reshape(
            plan.slots, plan.full, TILE_ROWS, LANES
        )
        for index in range(plan.full):
            out_ref[:, index * plan.blocks + block] = tile[:, index].astype(out_ref.dtype)
    for index in range(plan.tail_tiles):
        parts = []
        for part in range(plan.group):
            block = index * plan.group + part
            if block < plan.blocks:
                piece = product[plan.main_rows :, lane_block(block)]
                parts.append(piece.reshape(plan.slots, plan.tail, LANES))
        while len(parts) * plan.tail < TILE_ROWS:
            parts.append(jnp.zeros((plan.slots, min(plan.tail, TILE_ROWS - len(parts) * plan.tail), LANES), F32))
        tile = jnp.concatenate(parts, axis=1)
        out_ref[:, plan.full * plan.blocks + index] = tile.astype(out_ref.dtype)


def other_kernel(plan, packed_ref, acc_ref, gate_ref, up_ref, hidden_ref, rows_ref):
    unpack_rows(plan, packed_ref, rows_ref)
    first = pl.multiple_of((1 - lax.axis_index("rep")) * plan.feat, LANES)
    hid = gate_ref.shape[1]
    rows = rows_ref[...]
    gate = acc_ref[:, :hid] + jnp.dot(
        rows, gate_ref[pl.ds(first, plan.feat), :], preferred_element_type=F32
    )
    up = acc_ref[:, hid:] + jnp.dot(
        rows, up_ref[pl.ds(first, plan.feat), :], preferred_element_type=F32
    )
    hidden_ref[...] = (gate / (1.0 + jnp.exp(-gate)) * up).astype(BF16)


def down_product(plan, hidden_ref, down_ref):
    first = pl.multiple_of(lax.axis_index("rep") * plan.feat, LANES)
    return jnp.dot(
        hidden_ref[...], down_ref[:, pl.ds(first, plan.feat)], preferred_element_type=F32
    )


def down_own_kernel(plan, hidden_ref, down_ref, out_ref):
    out_ref[...] = down_product(plan, hidden_ref, down_ref)


def down_other_kernel(plan, hidden_ref, down_ref, mine_ref, out_ref):
    first = pl.multiple_of(lax.axis_index("rep") * plan.feat, LANES)
    half = (plan.blocks + 1) // 2 * LANES
    parts = []
    for start, size in ((0, half), (half, plan.feat - half)):
        if size:
            offset = pl.multiple_of(first + start, LANES)
            piece = jnp.dot(
                hidden_ref[...], down_ref[:, pl.ds(offset, size)], preferred_element_type=F32
            )
            parts.append(mine_ref[:, start : start + size] + piece)
    emit_packed(plan, jnp.concatenate(parts, axis=1), out_ref)


def combine_kernel(plan, pick_ref, column_ref, packed_ref, out_ref):
    for part in range(plan.parts):
        blocks = range(part, plan.blocks, plan.parts)
        tables = []
        for block in blocks:
            tiles = [index * plan.blocks + block for index in range(plan.full)]
            if plan.tail:
                tiles.append(plan.full * plan.blocks + block // plan.group)
            tables.append(jnp.concatenate([flat_tile(packed_ref[:, tile]) for tile in tiles], axis=0))
        table = jnp.concatenate(tables, axis=1)
        total = jnp.zeros((plan.tok, table.shape[1]), F32)
        for k in range(plan.choices):
            picked = jnp.dot(pick_ref[k * plan.parts + part], table, preferred_element_type=F32)
            total = total + column_ref[:, k : k + 1] * picked
        for index, block in enumerate(blocks):
            out_ref[:, lane_block(block)] = total[:, lane_block(index)].astype(BF16)


VMEM = pl.BlockSpec(memory_space=pltpu.VMEM)
ANY = pl.BlockSpec(memory_space=pltpu.HBM)


def call(kernel, in_specs, out_shape, flops, moved, limit, scratch=()):
    single = not isinstance(out_shape, (list, tuple))
    return pl.pallas_call(
        kernel,
        in_specs=in_specs,
        out_specs=VMEM if single else [VMEM] * len(out_shape),
        out_shape=out_shape,
        scratch_shapes=list(scratch),
        cost_estimate=pl.CostEstimate(flops=flops, bytes_accessed=moved, transcendentals=0),
        compiler_params=pltpu.CompilerParams(vmem_limit_bytes=limit),
    )


def body(tokens, expert_ids, gate_values, slot_expert, gate_weight, up_weight, down_weight):
    tok, choices = expert_ids.shape
    feat = tokens.shape[1]
    slots = slot_expert.shape[0]
    plan = Plan(tok, choices, feat, slots)
    weights = [gate_weight[0], up_weight[0], down_weight[0]]
    hid = weights[0].shape[1]
    gate_local, up_local, down_local = weights
    swap = [(0, 1), (1, 0)]
    packed_bytes = 2 * slots * plan.tiles * TILE_ROWS * LANES
    half_flops = 4 * plan.rows * feat * hid
    rows_scratch = pltpu.VMEM((plan.rows, feat), BF16)
    packed = jax.ShapeDtypeStruct(plan.packed, BF16)

    slot_row, ids, gates = slot_expert.reshape(1, slots), expert_ids.T, gate_values.T

    down_swapped = lax.ppermute(down_local, "rep", swap)
    warm = call(
        warm_kernel,
        [],
        jax.ShapeDtypeStruct((TILE_ROWS, LANES), F32),
        COVER_FLOPS,
        COVER_BYTES,
        1 * MIB,
    )()
    found = call(
        functools.partial(route_kernel, plan),
        [VMEM] * 3,
        jax.ShapeDtypeStruct((2 * choices, tok), jnp.int32),
        1 << 10,
        1 << 10,
        4 * MIB,
    )(warm, slot_row, ids)
    send = call(
        functools.partial(pack_kernel, plan), [VMEM] * 2, packed, COVER_FLOPS, COVER_BYTES, 8 * MIB
    )(found, tokens)
    arrived = exchange(send, slots)
    partner = lax.ppermute(arrived, "rep", swap)
    acc = call(
        functools.partial(own_kernel, plan),
        [VMEM] * 4,
        jax.ShapeDtypeStruct((plan.rows, 2 * hid), F32),
        1 << 10,
        1 << 10,
        8 * MIB,
        [rows_scratch],
    )(arrived, gate_local, up_local, down_local)
    picks, columns = call(
        functools.partial(select_kernel, plan),
        [VMEM, VMEM],
        [
            jax.ShapeDtypeStruct((choices * plan.parts, tok, plan.wide), BF16),
            jax.ShapeDtypeStruct((tok, choices), F32),
        ],
        1 << 10,
        1 << 10,
        4 * MIB,
    )(found, gates)
    hidden = call(
        functools.partial(other_kernel, plan),
        [VMEM] * 4,
        jax.ShapeDtypeStruct((plan.rows, hid), BF16),
        half_flops,
        packed_bytes + 8 * plan.rows * hid,
        8 * MIB,
        [rows_scratch],
    )(partner, acc, gate_local, up_local)
    received = lax.ppermute(hidden, "rep", swap)
    mine = call(
        functools.partial(down_own_kernel, plan),
        [VMEM] * 2,
        jax.ShapeDtypeStruct((plan.rows, feat), F32),
        2 * plan.wide * hid * feat,
        2 * packed_bytes,
        8 * MIB,
    )(hidden, down_local)
    result = call(
        functools.partial(down_other_kernel, plan),
        [VMEM] * 3,
        packed,
        2 * plan.wide * hid * feat,
        2 * packed_bytes,
        8 * MIB,
    )(received, down_swapped, mine)
    returned = exchange(result, slots)
    return call(
        functools.partial(combine_kernel, plan),
        [VMEM, VMEM, VMEM],
        jax.ShapeDtypeStruct((tok, feat), BF16),
        2 * tok * feat * plan.wide * choices,
        2 * packed_bytes,
        8 * MIB,
    )(picks, columns, returned)


def solution(mesh):
    assert mesh.shape["rep"] == 2
    return jax.shard_map(
        body,
        mesh=mesh,
        in_specs=(
            P(("groups", "ep"), "rep"),
            P(("groups", "ep"), None),
            P(("groups", "ep"), None),
            P(),
            P("ep", None, "rep"),
            P("ep", None, "rep"),
            P("ep", "rep", None),
        ),
        out_specs=P(("groups", "ep"), "rep"),
        check_vma=False,
    )
```
